16 devices in a mesh: tp: 2 (over z), cp: 8 (over y, x, core).
Axes of the slice: x: 2, y: 2, z: 2, core: 2. Of those that a mesh axis runs over, the one named last changes fastest.
Arguments:
- x_in: bfloat16 [8192, 1536], P('cp')
- positions: int32 [8192], P('cp')
- attn_gain: bfloat16 [2, 1536], replicated
- mlp_gain: bfloat16 [2, 1536], replicated
- w_query: bfloat16 [2, 1536, 1536], P(None, None, 'tp')
- b_query: bfloat16 [2, 1536], P(None, 'tp')
- w_key: bfloat16 [2, 1536, 256], P(None, None, 'tp')
- b_key: bfloat16 [2, 256], P(None, 'tp')
- w_value: bfloat16 [2, 1536, 256], P(None, None, 'tp')
- b_value: bfloat16 [2, 256], P(None, 'tp')
- w_out: bfloat16 [2, 1536, 1536], P(None, 'tp')
- w_gate: bfloat16 [2, 1536, 8960], P(None, None, 'tp')
- w_up: bfloat16 [2, 1536, 8960], P(None, None, 'tp')
- w_down: bfloat16 [2, 8960, 1536], P(None, 'tp')
Outputs:
- output 1: bfloat16 [8192, 1536], P('cp')
- output 2: bfloat16 [8192, 2, 128], P('cp', 'tp')
- output 3: bfloat16 [8192, 2, 128], P('cp', 'tp')
- output 4: bfloat16 [8192, 2, 128], P('cp', 'tp')
- output 5: bfloat16 [8192, 2, 128], P('cp', 'tp')
All inputs are finite; a program needn't handle non-finite values.
Results may differ from the reference program's by a relative error of at most 0.02.
Values are sent between devices in bfloat16 or wider.
A program may use at most 1 GiB of HBM per device.

```python
import jax
import jax.numpy as jnp
from jax import lax

TOKENS = 8192
HIDDEN = 1536
Q_HEADS = 12
KV_HEADS = 2
HEAD_DIM = 128
FFN_DIM = 8960
WINDOW = 4096


def setup_inputs(seed: int = 0) -> dict:
    key_list = jax.random.split(jax.random.key(seed), 14)
    q_width = Q_HEADS * HEAD_DIM
    kv_width = KV_HEADS * HEAD_DIM

    def normal_draw(key_idx, arr_shape, factor):
        return (jax.random.normal(key_list[key_idx], arr_shape, jnp.float32) * factor).astype(jnp.bfloat16)

    def gain_draw(key_idx):
        return jax.random.uniform(key_list[key_idx], (2, HIDDEN), jnp.float32, 0.5, 1.5).astype(jnp.bfloat16)

    pos_start = jax.random.randint(key_list[1], (), 0, 8192, jnp.int32)
    return {
        'x_in': normal_draw(0, (TOKENS, HIDDEN), 1.0),
        'positions': pos_start + jnp.arange(TOKENS, dtype=jnp.int32),
        'attn_gain': gain_draw(2),
        'mlp_gain': gain_draw(3),
        'w_query': normal_draw(4, (2, HIDDEN, q_width), 2.0 * HIDDEN ** -0.5),
        'b_query': normal_draw(5, (2, q_width), 0.5),
        'w_key': normal_draw(6, (2, HIDDEN, kv_width), 2.0 * HIDDEN ** -0.5),
        'b_key': normal_draw(7, (2, kv_width), 0.5),
        'w_value': normal_draw(8, (2, HIDDEN, kv_width), HIDDEN ** -0.5),
        'b_value': normal_draw(9, (2, kv_width), 0.5),
        'w_out': normal_draw(10, (2, q_width, HIDDEN), 2.0 * q_width ** -0.5),
        'w_gate': normal_draw(11, (2, HIDDEN, FFN_DIM), HIDDEN ** -0.5),
        'w_up': normal_draw(12, (2, HIDDEN, FFN_DIM), HIDDEN ** -0.5),
        'w_down': normal_draw(13, (2, FFN_DIM, HIDDEN), FFN_DIM ** -0.5),
    }


def rms_norm(hidden, gain):
    hidden_f = hidden.astype(jnp.float32)
    variance = jnp.mean(hidden_f * hidden_f, axis=-1, keepdims=True)
    return (hidden_f * lax.rsqrt(variance + 1e-6) * gain.astype(jnp.float32)).astype(jnp.bfloat16)


def rope_tables(positions):
    inv_freq = 1.0 / (1000000.0 ** (jnp.arange(0, HEAD_DIM, 2, dtype=jnp.float32) / HEAD_DIM))
    angles = positions.astype(jnp.float32)[:, None] * inv_freq[None, :]
    return jnp.cos(angles)[:, None, :], jnp.sin(angles)[:, None, :]


def apply_rope(proj_f, cos_tab, sin_tab):
    half_dim = proj_f.shape[-1] // 2
    first_half = proj_f[..., :half_dim]
    second_half = proj_f[..., half_dim:]
    return jnp.concatenate([first_half * cos_tab - second_half * sin_tab, second_half * cos_tab + first_half * sin_tab], axis=-1)


def project(normed, weight, bias_vec):
    return jnp.dot(normed, weight, preferred_element_type=jnp.float32) + bias_vec.astype(jnp.float32)


def attention(queries, key_cache, value_cache, window):
    group_size = Q_HEADS // KV_HEADS
    block_len = 128
    block_count = TOKENS // block_len
    q_blocks = queries.reshape(block_count, block_len, KV_HEADS, group_size, HEAD_DIM).astype(jnp.float32)
    keys_f = key_cache.astype(jnp.float32)
    values_f = value_cache.astype(jnp.float32)
    key_pos = jnp.arange(TOKENS)
    score_scale = HEAD_DIM ** -0.5

    def one_block(block_in):
        block_idx, q_blk = block_in
        query_pos = block_idx * block_len + jnp.arange(block_len)
        scores = jnp.einsum('qkgd,skd->qkgs', q_blk, keys_f) * score_scale
        allowed = (key_pos[None, :] <= query_pos[:, None]) & (key_pos[None, :] > query_pos[:, None] - window)
        scores = jnp.where(allowed[:, None, None, :], scores, -jnp.inf)
        probs = jax.nn.softmax(scores, axis=-1).astype(jnp.bfloat16).astype(jnp.float32)
        return jnp.einsum('qkgs,skd->qkgd', probs, values_f).astype(jnp.bfloat16)

    attn_out = lax.map(one_block, (jnp.arange(block_count), q_blocks))
    return attn_out.reshape(TOKENS, Q_HEADS * HEAD_DIM)


def reference(x_in, positions, attn_gain, mlp_gain, w_query, b_query, w_key, b_key, w_value, b_value, w_out, w_gate, w_up, w_down):
    cos_tab, sin_tab = rope_tables(positions)
    hidden = x_in
    caches = []
    for layer_idx, window in ((0, TOKENS), (1, WINDOW)):
        normed = rms_norm(hidden, attn_gain[layer_idx])
        queries = apply_rope(project(normed, w_query[layer_idx], b_query[layer_idx]).reshape(TOKENS, Q_HEADS, HEAD_DIM), cos_tab, sin_tab).astype(jnp.bfloat16)
        key_cache = apply_rope(project(normed, w_key[layer_idx], b_key[layer_idx]).reshape(TOKENS, KV_HEADS, HEAD_DIM), cos_tab, sin_tab).astype(jnp.bfloat16)
        value_cache = project(normed, w_value[layer_idx], b_value[layer_idx]).astype(jnp.bfloat16).reshape(TOKENS, KV_HEADS, HEAD_DIM)
        attn_out = attention(queries, key_cache, value_cache, window)
        hidden = (hidden.astype(jnp.float32) + jnp.dot(attn_out, w_out[layer_idx], preferred_element_type=jnp.float32)).astype(jnp.bfloat16)
        normed = rms_norm(hidden, mlp_gain[layer_idx])
        gate_proj = jnp.dot(normed, w_gate[layer_idx], preferred_element_type=jnp.float32)
        up_proj = jnp.dot(normed, w_up[layer_idx], preferred_element_type=jnp.float32)
        activated = (jax.nn.silu(gate_proj) * up_proj).astype(jnp.bfloat16)
        hidden = (hidden.astype(jnp.float32) + jnp.dot(activated, w_down[layer_idx], preferred_element_type=jnp.float32)).astype(jnp.bfloat16)
        caches.append(key_cache)
        caches.append(value_cache)
    return (hidden, caches[0], caches[1], caches[2], caches[3])
```

```python
import functools

import jax
import jax.numpy as jnp
from jax import lax
from jax.experimental import pallas as pl
from jax.experimental.pallas import tpu as pltpu
from jax.sharding import PartitionSpec as P

HEAD_DIM = 128
WINDOW = 4096
SCORE_SCALE = (HEAD_DIM ** -0.5) * 1.4426950408889634
MIB = 1024 * 1024


def rms_rows(hidden_f, gain_f):
    variance = jnp.mean(hidden_f * hidden_f, axis=-1, keepdims=True)
    return (hidden_f * lax.rsqrt(variance + 1e-6) * gain_f).astype(jnp.bfloat16)


def qkv_kernel(x_ref, gain_ref, wq_ref, wk_ref, wv_ref, bq_ref, bk_ref, bv_ref, cos_ref, sin_ref, q_ref, k_ref, v_ref):
    normed = rms_rows(x_ref[...].astype(jnp.float32), gain_ref[...].astype(jnp.float32))
    cos_tab = cos_ref[...]
    sin_tab = sin_ref[...]

    def rope(block):
        return (block * cos_tab + pltpu.roll(block, HEAD_DIM // 2, 1) * sin_tab).astype(jnp.bfloat16)

    k_f = jnp.dot(normed, wk_ref[...], preferred_element_type=jnp.float32) + bk_ref[...].astype(jnp.float32)
    k_ref[...] = rope(k_f)
    v_f = jnp.dot(normed, wv_ref[...], preferred_element_type=jnp.float32) + bv_ref[...].astype(jnp.float32)
    v_ref[...] = v_f.astype(jnp.bfloat16)
    q_f = jnp.dot(normed, wq_ref[...], preferred_element_type=jnp.float32) + bq_ref[...].astype(jnp.float32)
    for head in range(q_ref.shape[1] // HEAD_DIM):
        cols = slice(head * HEAD_DIM, (head + 1) * HEAD_DIM)
        q_ref[:, cols] = rope(q_f[:, cols])


def qkv(layer, x, gain, wq, wk, wv, bq, bk, bv, cos_tab, sin_tab, row0):
    rows, width = x.shape
    q_cols = wq.shape[2]
    block = min(rows, 256)
    tab0 = row0 // block

    def whole(w):
        return pl.BlockSpec((None,) + w.shape[1:], lambda i: (layer, 0, 0))

    def table():
        return pl.BlockSpec((block, HEAD_DIM), lambda i: (i + tab0, 0))

    def out(cols):
        return pl.BlockSpec((block, cols), lambda i: (i, 0))

    return pl.pallas_call(
        qkv_kernel,
        grid=(rows // block,),
        in_specs=[out(width)] + [whole(w) for w in (gain, wq, wk, wv, bq, bk, bv)] + [table(), table()],
        out_specs=[out(q_cols), out(HEAD_DIM), out(HEAD_DIM)],
        out_shape=[jax.ShapeDtypeStruct((rows, c), jnp.bfloat16) for c in (q_cols, HEAD_DIM, HEAD_DIM)],
        compiler_params=pltpu.CompilerParams(vmem_limit_bytes=32 * MIB),
        cost_estimate=pl.CostEstimate(flops=2 * rows * width * (q_cols + 256), bytes_accessed=rows * width * 4 + width * 2048, transcendentals=0),
        name="qkv",
    )(x, gain, wq, wk, wv, bq, bk, bv, cos_tab, sin_tab)


def attn_kernel(start_ref, q_ref, k_ref, v_ref, o_ref, m_sc, l_sc, acc_sc, *, bk, sub, window):
    bq = q_ref.shape[0]
    heads = q_ref.shape[1] // HEAD_DIM
    t0 = start_ref[0] + pl.program_id(0) * bq
    m_sc[...] = jnp.full(m_sc.shape, -1e30, jnp.float32)
    l_sc[...] = jnp.zeros(l_sc.shape, jnp.float32)
    acc_sc[...] = jnp.zeros(acc_sc.shape, jnp.float32)
    units = [(h, r) for h in range(heads) for r in range(0, bq, sub)]

    def block(b, masked):
        kst = pl.multiple_of(b * bk, bk)
        kb = k_ref[pl.ds(kst, bk), :]
        vb = v_ref[pl.ds(kst, bk), :]

        def scores(unit):
            h, r = unit
            qh = q_ref[r:r + sub, h * HEAD_DIM:(h + 1) * HEAD_DIM]
            return lax.dot_general(qh, kb, (((1,), (1,)), ((), ())), preferred_element_type=jnp.float32)

        def soft(unit, s):
            h, r = unit
            sl = pl.ds(r, sub)
            if masked:
                rows = t0 + r + lax.broadcasted_iota(jnp.int32, (sub, bk), 0)
                cols = kst + lax.broadcasted_iota(jnp.int32, (sub, bk), 1)
                keep = (cols <= rows) & (cols > rows - window)
                s = jnp.where(keep, s, -1e30)
            m_old = m_sc[h, sl]
            m_new = jnp.maximum(m_old, jnp.max(s, axis=1, keepdims=True) * SCORE_SCALE)
            m_sc[h, sl] = m_new
            alpha = jnp.exp2(m_old - m_new)
            p = jnp.exp2(s * SCORE_SCALE - jnp.tile(m_new, (1, bk // HEAD_DIM)))
            if masked:
                p = jnp.where(keep, p, 0.0)
            parts = [p[:, j:j + HEAD_DIM] for j in range(0, bk, HEAD_DIM)]
            while len(parts) > 1:
                parts = [parts[i] + parts[i + 1] for i in range(0, len(parts), 2)]
            l_sc[h, sl] = l_sc[h, sl] * alpha + parts[0]
            return p.astype(jnp.bfloat16), alpha

        def weigh(unit, p, alpha):
            h, r = unit
            sl = pl.ds(r, sub)
            acc_sc[h, sl] = acc_sc[h, sl] * alpha + jnp.dot(p, vb, preferred_element_type=jnp.float32)

        n = len(units)
        s_of, p_of = {}, {}
        for i in range(n + 2):
            if i < n:
                s_of[i] = scores(units[i])
            if i >= 2:
                weigh(units[i - 2], *p_of.pop(i - 2))
            if 1 <= i <= n:
                p_of[i - 1] = soft(units[i - 1], s_of.pop(i - 1))

    lo = jnp.maximum(t0 - window + 1, 0) // bk
    lo_full = (jnp.maximum(t0 + bq - window, 0) + bk - 1) // bk
    hi_full = (t0 + 1) // bk
    hi = (t0 + bq + bk - 1) // bk

    def masked_block(b, carry):
        block(b, True)
        return carry

    def full_block(b, carry):
        block(b, False)
        return carry

    lax.fori_loop(lo, lo_full, masked_block, 0)
    lax.fori_loop(lo_full, hi_full, full_block, 0)
    lax.fori_loop(hi_full, hi, masked_block, 0)
    for h in range(heads):
        total = jnp.sum(l_sc[h], axis=1, keepdims=True)
        o_ref[:, h * HEAD_DIM:(h + 1) * HEAD_DIM] = (acc_sc[h] / total).astype(jnp.bfloat16)


def attention(q, k_all, v_all, start, row0, rows, window):
    cols = q.shape[1]
    keys = k_all.shape[0]
    bq = min(rows, 512)
    heads = cols // HEAD_DIM
    kern = functools.partial(attn_kernel, bk=512, sub=256, window=window)
    blk0 = row0 // bq
    return pl.pallas_call(
        kern,
        grid_spec=pltpu.PrefetchScalarGridSpec(
            num_scalar_prefetch=1,
            grid=(rows // bq,),
            in_specs=[
                pl.BlockSpec((bq, cols), lambda i, s: (i + blk0, 0)),
                pl.BlockSpec((keys, HEAD_DIM), lambda i, s: (0, 0)),
                pl.BlockSpec((keys, HEAD_DIM), lambda i, s: (0, 0)),
            ],
            out_specs=pl.BlockSpec((bq, cols), lambda i, s: (i, 0)),
            scratch_shapes=[pltpu.VMEM((heads, bq, HEAD_DIM), jnp.float32)] * 3,
        ),
        out_shape=jax.ShapeDtypeStruct((rows, cols), jnp.bfloat16),
        compiler_params=pltpu.CompilerParams(vmem_limit_bytes=48 * MIB),
        cost_estimate=pl.CostEstimate(flops=8 * rows * cols * min(window, keys), bytes_accessed=rows * cols * 4 + keys * 512, transcendentals=0),
        name="attn",
    )(start, q, k_all, v_all)


def out_kernel(place_ref, o_own_ref, o_peer_ref, x_ref, gain_ref, w_own_hbm, w_z_hbm, w_d_hbm, x1_ref, h2_ref, w_full, o_full, sems, *, layer):
    half = o_own_ref.shape[1]
    quarter = half // 2
    own0 = pl.multiple_of(place_ref[0] * half, half)
    peer0 = pl.multiple_of((1 - place_ref[0]) * half, half)
    core = place_ref[1]

    @pl.when(pl.program_id(0) == 0)
    def _():
        zrow = pl.multiple_of(peer0 + core * quarter, quarter)
        drow = pl.multiple_of(peer0 + (1 - core) * quarter, quarter)
        copies = [
            pltpu.make_async_copy(w_own_hbm.at[layer], w_full.at[pl.ds(own0, half)], sems.at[0]),
            pltpu.make_async_copy(w_z_hbm.at[layer], w_full.at[pl.ds(zrow, quarter)], sems.at[1]),
            pltpu.make_async_copy(w_d_hbm.at[layer], w_full.at[pl.ds(drow, quarter)], sems.at[2]),
        ]
        for copy in copies:
            copy.start()
        for copy in copies:
            copy.wait()

    o_full[:, pl.ds(own0, half)] = o_own_ref[...]
    o_full[:, pl.ds(peer0, half)] = o_peer_ref[...]
    prod = jnp.dot(o_full[...], w_full[...], preferred_element_type=jnp.float32)
    x1 = (x_ref[...].astype(jnp.float32) + prod).astype(jnp.bfloat16)
    x1_ref[...] = x1
    h2_ref[...] = rms_rows(x1.astype(jnp.float32), gain_ref[...].astype(jnp.float32))


def out_project(layer, place, o_own, o_peer, x, x_row0, gain, w_own, w_z, w_d):
    rows, half = o_own.shape
    width = x.shape[1]
    block = min(rows, 256)
    xb = x_row0 // block

    def rowspec(cols, off=0):
        return pl.BlockSpec((block, cols), lambda i, s: (i + off, 0))

    return pl.pallas_call(
        functools.partial(out_kernel, layer=layer),
        grid_spec=pltpu.PrefetchScalarGridSpec(
            num_scalar_prefetch=1,
            grid=(rows // block,),
            in_specs=[
                rowspec(half), rowspec(half), rowspec(width, xb),
                pl.BlockSpec((None, 1, width), lambda i, s: (layer, 0, 0)),
                pl.BlockSpec(memory_space=pl.ANY), pl.BlockSpec(memory_space=pl.ANY), pl.BlockSpec(memory_space=pl.ANY),
            ],
            out_specs=[rowspec(width), rowspec(width)],
            scratch_shapes=[pltpu.VMEM((2 * half, width), jnp.bfloat16), pltpu.VMEM((block, 2 * half), jnp.bfloat16), pltpu.SemaphoreType.DMA((3,))],
        ),
        out_shape=[jax.ShapeDtypeStruct((rows, width), jnp.bfloat16)] * 2,
        compiler_params=pltpu.CompilerParams(vmem_limit_bytes=32 * MIB),
        cost_estimate=pl.CostEstimate(flops=4 * rows * half * width, bytes_accessed=rows * width * 10 + 4 * half * width, transcendentals=0),
        name="outproj",
    )(place, o_own, o_peer, x, gain, w_own, w_z, w_d)


def mlp_kernel(h_ref, wg_ref, wu_ref, wd_ref, out_ref, acc):
    step = pl.program_id(0)
    normed = h_ref[...]
    gate = jnp.dot(normed, wg_ref[...], preferred_element_type=jnp.float32)
    up = jnp.dot(normed, wu_ref[...], preferred_element_type=jnp.float32)
    act = (gate * jax.nn.sigmoid(gate) * up).astype(jnp.bfloat16)
    part = jnp.dot(act, wd_ref[...], preferred_element_type=jnp.float32)

    @pl.when(step == 0)
    def _():
        acc[...] = part

    @pl.when(step > 0)
    def _():
        acc[...] += part

    @pl.when(step == pl.num_programs(0) - 1)
    def _():
        out_ref[...] = acc[...].astype(jnp.bfloat16)


def mlp(layer, h2, row0, rows, wg, wu, wd):
    width = h2.shape[1]
    cols = wg.shape[2]
    tile = 640
    blk = row0 // rows
    return pl.pallas_call(
        mlp_kernel,
        grid=(cols // tile,),
        in_specs=[
            pl.BlockSpec((rows, width), lambda j: (blk, 0)),
            pl.BlockSpec((None, width, tile), lambda j: (layer, 0, j)),
            pl.BlockSpec((None, width, tile), lambda j: (layer, 0, j)),
            pl.BlockSpec((None, tile, width), lambda j: (layer, j, 0)),
        ],
        out_specs=pl.BlockSpec((rows, width), lambda j: (0, 0)),
        out_shape=jax.ShapeDtypeStruct((rows, width), jnp.bfloat16),
        scratch_shapes=[pltpu.VMEM((rows, width), jnp.float32)],
        compiler_params=pltpu.CompilerParams(vmem_limit_bytes=48 * MIB),
        cost_estimate=pl.CostEstimate(flops=6 * rows * width * cols, bytes_accessed=6 * width * cols, transcendentals=0),
        name="mlp",
    )(h2, wg, wu, wd)


def solution(mesh):
    cp_size = mesh.shape["cp"]
    z_swap = [(0, 1), (1, 0)]
    core_swap = [(i, i ^ 1) for i in range(cp_size)]
    row_cuts = ((0, 512), (512, 256), (768, 256))

    def local_step(x_in, positions, attn_gain, mlp_gain, w_query, b_query, w_key, b_key, w_value, b_value, w_out, w_gate, w_up, w_down):
        block_dev = x_in.shape[0]
        tp = lax.axis_index("tp")
        cp = lax.axis_index("cp")
        start = cp * block_dev
        inv_freq = 1.0 / (1000000.0 ** (jnp.arange(0, HEAD_DIM, 2, dtype=jnp.float32) / HEAD_DIM))
        angles = positions.astype(jnp.float32)[:, None] * inv_freq[None, :]
        cos_half, sin_half = jnp.cos(angles), jnp.sin(angles)
        cos_tab = jnp.concatenate([cos_half, cos_half], axis=1)
        sin_tab = jnp.concatenate([-sin_half, sin_half], axis=1)
        row = lambda a: a[:, None, :]
        attn_gain, mlp_gain, b_query, b_key, b_value = (row(a) for a in (attn_gain, mlp_gain, b_query, b_key, b_value))

        quarter = w_out.shape[1] // 2
        w_half = lax.dynamic_slice_in_dim(w_out, (cp % 2) * quarter, quarter, axis=1)
        w_z = lax.ppermute(w_half, "tp", z_swap)
        w_d = None
        place = jnp.stack([tp, cp % 2]).astype(jnp.int32)

        hidden = [(0, block_dev, x_in, 0)]
        caches = []
        for layer, window in ((0, block_dev * cp_size), (1, WINDOW)):
            parts = [qkv(layer, h, attn_gain, w_query, w_key, w_value, b_query, b_key, b_value, cos_tab, sin_tab, r0) for r0, n, h, _ in hidden]
            q, k, v = (jnp.concatenate(p, axis=0) if len(p) > 1 else p[0] for p in zip(*parts))
            k_all = lax.all_gather(k, "cp", axis=0, tiled=True)
            v_all = lax.all_gather(v, "cp", axis=0, tiled=True)
            outs = []
            for r0, n in row_cuts:
                o = attention(q, k_all, v_all, jnp.reshape(start + r0, (1,)).astype(jnp.int32), r0, n, window)
                if w_d is None and r0 > 0:
                    o, w_z = lax.optimization_barrier((o, w_z))
                    w_d = lax.ppermute(w_z, "cp", core_swap)
                outs.append((r0, n, o, lax.ppermute(o, "tp", z_swap)))
            new_hidden = []
            for r0, n, o, o_peer in outs:
                if layer == 0:
                    src, off = x_in, r0
                else:
                    mine = [h for s, _, h, _ in hidden if r0 <= s < r0 + n]
                    src, off = (mine[0] if len(mine) == 1 else jnp.concatenate(mine, axis=0)), 0
                x1, h2 = out_project(layer, place, o, o_peer, src, off, mlp_gain, w_out, w_z, w_d)
                for c in range(0, n, 256):
                    part = mlp(layer, h2, c, 256, w_gate, w_up, w_down)
                    other = lax.ppermute(part, "tp", z_swap)
                    total = part.astype(jnp.float32) + other.astype(jnp.float32)
                    nxt = (x1[c:c + 256].astype(jnp.float32) + total).astype(jnp.bfloat16)
                    new_hidden.append((r0 + c, 256, nxt, 0))
            hidden = new_hidden
            caches.append(k[:, None, :])
            caches.append(v[:, None, :])
        x_out = jnp.concatenate([h for _, _, h, _ in hidden], axis=0)
        return x_out, caches[0], caches[1], caches[2], caches[3]

    weight_col = P(None, None, "tp")
    bias_col = P(None, "tp")
    weight_row = P(None, "tp", None)
    replicated = P(None, None)
    cache_spec = P("cp", "tp", None)
    in_specs = (P("cp", None), P("cp"), replicated, replicated, weight_col, bias_col, weight_col, bias_col, weight_col, bias_col, weight_row, weight_col, weight_col, weight_row)
    out_specs = (P("cp", None), cache_spec, cache_spec, cache_spec, cache_spec)
    return jax.shard_map(local_step, mesh=mesh, in_specs=in_specs, out_specs=out_specs, check_vma=False)
```

```python
import functools

import jax
import jax.numpy as jnp
from jax import lax
from jax.experimental import pallas as pl
from jax.experimental.pallas import tpu as pltpu
from jax.sharding import PartitionSpec as P

HEAD_DIM = 128
WINDOW = 4096
SCORE_SCALE = (HEAD_DIM ** -0.5) * 1.4426950408889634
MIB = 1024 * 1024
MESH = pl.DeviceIdType.MESH


def rms_rows(hidden_f, gain_f):
    variance = jnp.mean(hidden_f * hidden_f, axis=-1, keepdims=True)
    return (hidden_f * lax.rsqrt(variance + 1e-6) * gain_f).astype(jnp.bfloat16)


def qkv_kernel(x_ref, gain_ref, wq_ref, wk_ref, wv_ref, bq_ref, bk_ref, bv_ref, cos_ref, sin_ref, q_ref, k_ref, v_ref, kv_ref):
    normed = rms_rows(x_ref[...].astype(jnp.float32), gain_ref[...].astype(jnp.float32))
    cos_tab = cos_ref[...]
    sin_tab = sin_ref[...]

    def rope(block):
        return (block * cos_tab + pltpu.roll(block, HEAD_DIM // 2, 1) * sin_tab).astype(jnp.bfloat16)

    k_f = jnp.dot(normed, wk_ref[...], preferred_element_type=jnp.float32) + bk_ref[...].astype(jnp.float32)
    k_b = rope(k_f)
    k_ref[...] = k_b
    kv_ref[:, :HEAD_DIM] = k_b
    v_f = jnp.dot(normed, wv_ref[...], preferred_element_type=jnp.float32) + bv_ref[...].astype(jnp.float32)
    v_b = v_f.astype(jnp.bfloat16)
    v_ref[...] = v_b
    kv_ref[:, HEAD_DIM:] = v_b
    q_f = jnp.dot(normed, wq_ref[...], preferred_element_type=jnp.float32) + bq_ref[...].astype(jnp.float32)
    for head in range(q_ref.shape[1] // HEAD_DIM):
        cols = slice(head * HEAD_DIM, (head + 1) * HEAD_DIM)
        q_ref[:, cols] = rope(q_f[:, cols])


def qkv(layer, x, gain, wq, wk, wv, bq, bk, bv, cos_tab, sin_tab):
    rows, width = x.shape
    q_cols = wq.shape[2]
    block = min(rows, 256)

    def whole(w):
        return pl.BlockSpec((None,) + w.shape[1:], lambda i: (layer, 0, 0))

    def table():
        return pl.BlockSpec((block, HEAD_DIM), lambda i: (i, 0))

    def out(cols):
        return pl.BlockSpec((block, cols), lambda i: (i, 0))

    return pl.pallas_call(
        qkv_kernel,
        grid=(rows // block,),
        in_specs=[out(width)] + [whole(w) for w in (gain, wq, wk, wv, bq, bk, bv)] + [table(), table()],
        out_specs=[out(c) for c in (q_cols, HEAD_DIM, HEAD_DIM, 2 * HEAD_DIM)],
        out_shape=[jax.ShapeDtypeStruct((rows, c), jnp.bfloat16) for c in (q_cols, HEAD_DIM, HEAD_DIM, 2 * HEAD_DIM)],
        compiler_params=pltpu.CompilerParams(vmem_limit_bytes=32 * MIB),
        cost_estimate=pl.CostEstimate(flops=2 * rows * width * (q_cols + 256), bytes_accessed=rows * width * 4 + width * 2048, transcendentals=0),
        name="qkv",
    )(x, gain, wq, wk, wv, bq, bk, bv, cos_tab, sin_tab)


def attn_kernel(*refs, bq, window_blocks, with_w):
    refs = list(refs)
    q_ref, kv_ref = refs[:2]; refs = refs[2:]
    w_out = refs.pop(0) if with_w else None
    o_ref, o_peer = refs[:2]; refs = refs[2:]
    w_peer = refs.pop(0) if with_w else None
    kv_buf, m_sc, l_sc, acc_sc, send_sems, recv_sems, o_send, o_recv, w_send, w_recv = refs
    rows = q_ref.shape[0]
    heads = q_ref.shape[1] // HEAD_DIM
    cp = lax.axis_index("cp")
    core, xpos, ypos = lax.rem(cp, 2), lax.rem(lax.div(cp, 2), 2), lax.div(cp, 4)
    to_mate, to_x, to_y = 1 - 2 * core, 2 - 4 * xpos, 4 - 8 * ypos
    mate, xnb, ynb, diag = cp + to_mate, cp + to_x, cp + to_y, cp + to_x + to_y
    half = rows // 2

    peer = 1 - lax.axis_index("tp")
    at_cp = lambda i: {"cp": i}
    whole = pl.ds(0, rows)

    def kv_copy(i, src, slot, part, dev):
        return pltpu.make_async_remote_copy(src_ref=src, dst_ref=kv_buf.at[slot, part], send_sem=send_sems.at[i], recv_sem=recv_sems.at[i], device_id=at_cp(dev), device_id_type=MESH)

    first, last = pl.ds(0, half), pl.ds(half, half)
    kv_copies = [
        kv_copy(0, kv_ref, cp, whole, mate),
        kv_copy(1, kv_ref, cp, whole, xnb),
        kv_copy(2, kv_ref, cp, whole, ynb),
        kv_copy(3, kv_buf.at[xnb], xnb, whole, mate),
        kv_copy(4, kv_buf.at[ynb], ynb, whole, mate),
        kv_copy(5, kv_buf.at[xnb, first], xnb, first, ynb),
        kv_copy(6, kv_buf.at[ynb, last], ynb, last, xnb),
        kv_copy(7, kv_buf.at[diag], diag, whole, mate),
    ]
    if with_w:
        quarter = w_out.shape[1] // 2
        mine = pl.ds(pl.multiple_of(core * quarter, quarter), quarter)
        w_z = pltpu.make_async_remote_copy(src_ref=w_out.at[:, mine], dst_ref=w_peer.at[:, mine], send_sem=w_send.at[0], recv_sem=w_recv.at[0], device_id={"tp": peer}, device_id_type=MESH)
        w_d = pltpu.make_async_remote_copy(src_ref=w_peer.at[:, mine], dst_ref=w_peer.at[:, mine], send_sem=w_send.at[1], recv_sem=w_recv.at[1], device_id=at_cp(mate), device_id_type=MESH)

    barrier = pltpu.get_barrier_semaphore()
    for dev in (at_cp(mate), at_cp(xnb), at_cp(ynb), {"tp": peer}):
        pl.semaphore_signal(barrier, inc=1, device_id=dev, device_id_type=MESH)
    pl.semaphore_wait(barrier, 4)
    for copy in kv_copies[:3]:
        copy.start()
    if with_w:
        w_z.start()

    def o_copy(qb):
        part = pl.ds(pl.multiple_of(qb * bq, bq), bq)
        return pltpu.make_async_remote_copy(src_ref=o_ref.at[part], dst_ref=o_peer.at[part], send_sem=o_send.at[qb], recv_sem=o_recv.at[qb], device_id={"tp": peer}, device_id_type=MESH)

    def block(q0, kb, vb, keep):
        bk = kb.shape[0]

        def scores(h):
            qh = q_ref[pl.ds(q0, bq), h * HEAD_DIM:(h + 1) * HEAD_DIM]
            return lax.dot_general(qh, kb, (((1,), (1,)), ((), ())), preferred_element_type=jnp.float32)

        def soft(h, s):
            if keep is not None:
                s = jnp.where(keep, s, -1e30)
            m_old = m_sc[h]
            m_new = jnp.maximum(m_old, jnp.max(s, axis=1, keepdims=True) * SCORE_SCALE)
            m_sc[h] = m_new
            alpha = jnp.exp2(m_old - m_new)
            p = jnp.exp2(s * SCORE_SCALE - jnp.tile(m_new, (1, bk // HEAD_DIM)))
            if keep is not None:
                p = jnp.where(keep, p, 0.0)
            parts = [p[:, j:j + HEAD_DIM] for j in range(0, bk, HEAD_DIM)]
            while len(parts) > 1:
                parts = [parts[i] + parts[i + 1] for i in range(0, len(parts), 2)]
            l_sc[h] = l_sc[h] * alpha + parts[0]
            return p.astype(jnp.bfloat16), alpha

        def weigh(h, p, alpha):
            acc_sc[h] = acc_sc[h] * alpha + jnp.dot(p, vb, preferred_element_type=jnp.float32)

        s_of, p_of = {}, {}
        for i in range(heads + 2):
            if i < heads:
                s_of[i] = scores(i)
            if i >= 2:
                weigh(i - 2, *p_of.pop(i - 2))
            if 1 <= i <= heads:
                p_of[i - 1] = soft(i - 1, s_of.pop(i - 1))

    def split(ref, *at):
        return ref[at + (slice(None, HEAD_DIM),)], ref[at + (slice(HEAD_DIM, None),)]

    def q_block(qb, carry):
        q0 = pl.multiple_of(qb * bq, bq)
        m_sc[...] = jnp.full(m_sc.shape, -1e30, jnp.float32)
        l_sc[...] = jnp.zeros(l_sc.shape, jnp.float32)
        acc_sc[...] = jnp.zeros(acc_sc.shape, jnp.float32)
        row = lax.broadcasted_iota(jnp.int32, (bq, bq), 0)
        col = lax.broadcasted_iota(jnp.int32, (bq, bq), 1)

        def own_part(j, c):
            block(q0, *split(kv_ref, pl.ds(pl.multiple_of(j * bq, bq), bq)), None)
            return c

        block(q0, *split(kv_ref, pl.ds(q0, bq)), col <= row)
        lax.fori_loop(0, qb, own_part, 0)

        def step_body(step, c):
            src = cp + lax.rem(step, 2) * to_mate + lax.rem(lax.div(step, 2), 2) * to_x + lax.div(step, 4) * to_y
            @pl.when(qb == 0)
            def _():
                @pl.when(step == 1)
                def _():
                    kv_copies[0].wait_recv()

                @pl.when(step == 2)
                def _():
                    kv_copies[1].wait_recv()
                    kv_copies[3].start()
                    kv_copies[5].start()
                    kv_copies[2].wait_recv()
                    kv_copies[4].start()
                    kv_copies[6].start()

                @pl.when(step == 3)
                def _():
                    kv_copies[3].wait_recv()

                @pl.when(step == 5)
                def _():
                    kv_copies[4].wait_recv()

                @pl.when(step == 6)
                def _():
                    kv_copies[5].wait_recv()
                    kv_copies[6].wait_recv()
                    kv_copies[7].start()

                @pl.when(step == 7)
                def _():
                    kv_copies[7].wait_recv()
            @pl.when((src < cp) & (src > cp - window_blocks))
            def _():
                block(q0, *split(kv_buf, src, slice(None)), None)

            if window_blocks < 8:
                @pl.when(src == cp - window_blocks)
                def _():
                    block(q0, *split(kv_buf, src, pl.ds(q0, bq)), col > row)

                    def edge_part(j, cc):
                        block(q0, *split(kv_buf, src, pl.ds(pl.multiple_of(j * bq, bq), bq)), None)
                        return cc

                    lax.fori_loop(qb + 1, rows // bq, edge_part, 0)
            return c

        lax.fori_loop(1, 8, step_body, 0)
        for h in range(heads):
            total = jnp.sum(l_sc[h], axis=1, keepdims=True)
            o_ref[pl.ds(q0, bq), h * HEAD_DIM:(h + 1) * HEAD_DIM] = (acc_sc[h] / total).astype(jnp.bfloat16)
        o_copy(qb).start()
        if with_w:
            @pl.when(qb == 0)
            def _():
                w_z.wait_recv()
                w_d.start()
        return carry

    lax.fori_loop(0, rows // bq, q_block, 0)
    for copy in kv_copies:
        copy.wait_send()
    if with_w:
        w_z.wait_send()
        w_d.wait()
    for qb in range(rows // bq):
        o_copy(qb).wait()

def attention(q, kv, w_out, window_blocks, bq, cid):
    rows, cols = q.shape
    heads = cols // HEAD_DIM
    with_w = w_out is not None
    bf = jnp.bfloat16
    vm = pl.BlockSpec(memory_space=pltpu.VMEM)
    anys = pl.BlockSpec(memory_space=pl.ANY)
    nq = rows // bq
    outs = [jax.ShapeDtypeStruct((rows, cols), bf), jax.ShapeDtypeStruct((rows, cols), bf)]
    if with_w: outs.append(jax.ShapeDtypeStruct(w_out.shape, bf))
    dma = pltpu.SemaphoreType.DMA
    return pl.pallas_call(
        functools.partial(attn_kernel, bq=bq, window_blocks=window_blocks, with_w=with_w),
        in_specs=[vm, vm] + [anys] * with_w,
        out_specs=[vm, anys] + [anys] * with_w,
        out_shape=outs,
        scratch_shapes=[pltpu.VMEM((8, rows, 2 * HEAD_DIM), bf)] + [pltpu.VMEM((heads, bq, HEAD_DIM), jnp.float32)] * 3
        + [dma((8,)), dma((8,)), dma((nq,)), dma((nq,)), dma((2,)), dma((2,))],
        compiler_params=pltpu.CompilerParams(vmem_limit_bytes=48 * MIB, collective_id=cid, has_side_effects=True),
        cost_estimate=pl.CostEstimate(flops=16 * rows * rows * cols, bytes_accessed=rows * cols * 6, transcendentals=0),
        name="attn",
    )(q, kv, *([w_out] if with_w else []))


def out_kernel(place_ref, o_own_ref, o_peer_ref, x_ref, gain_ref, w_own_hbm, w_peer_hbm, x1_ref, h2_ref, w_full, o_full, sems, *, layer):
    half = o_own_ref.shape[1]
    own0 = pl.multiple_of(place_ref[0] * half, half)
    peer0 = pl.multiple_of((1 - place_ref[0]) * half, half)

    @pl.when(pl.program_id(0) == 0)
    def _():
        copies = [
            pltpu.make_async_copy(w_own_hbm.at[layer], w_full.at[pl.ds(own0, half)], sems.at[0]),
            pltpu.make_async_copy(w_peer_hbm.at[layer], w_full.at[pl.ds(peer0, half)], sems.at[1]),
        ]
        for copy in copies:
            copy.start()
        for copy in copies:
            copy.wait()

    o_full[:, pl.ds(own0, half)] = o_own_ref[...]
    o_full[:, pl.ds(peer0, half)] = o_peer_ref[...]
    prod = jnp.dot(o_full[...], w_full[...], preferred_element_type=jnp.float32)
    x1 = (x_ref[...].astype(jnp.float32) + prod).astype(jnp.bfloat16)
    x1_ref[...] = x1
    h2_ref[...] = rms_rows(x1.astype(jnp.float32), gain_ref[...].astype(jnp.float32))


def out_project(layer, place, o_own, o_peer, x, gain, w_own, w_peer):
    rows, half = o_own.shape
    width = x.shape[1]
    block = min(rows, 256)

    def rowspec(cols):
        return pl.BlockSpec((block, cols), lambda i, s: (i, 0))

    return pl.pallas_call(
        functools.partial(out_kernel, layer=layer),
        grid_spec=pltpu.PrefetchScalarGridSpec(
            num_scalar_prefetch=1,
            grid=(rows // block,),
            in_specs=[
                rowspec(half), rowspec(half), rowspec(width),
                pl.BlockSpec((None, 1, width), lambda i, s: (layer, 0, 0)),
                pl.BlockSpec(memory_space=pl.ANY), pl.BlockSpec(memory_space=pl.ANY),
            ],
            out_specs=[rowspec(width), rowspec(width)],
            scratch_shapes=[pltpu.VMEM((2 * half, width), jnp.bfloat16), pltpu.VMEM((block, 2 * half), jnp.bfloat16), pltpu.SemaphoreType.DMA((2,))],
        ),
        out_shape=[jax.ShapeDtypeStruct((rows, width), jnp.bfloat16)] * 2,
        compiler_params=pltpu.CompilerParams(vmem_limit_bytes=32 * MIB),
        cost_estimate=pl.CostEstimate(flops=4 * rows * half * width, bytes_accessed=rows * width * 10 + 4 * half * width, transcendentals=0),
        name="outproj",
    )(place, o_own, o_peer, x, gain, w_own, w_peer)


def mlp_kernel(h_ref, x1_hbm, wg_hbm, wu_hbm, wd_hbm, out_hbm, wg, wu, wd, send, recv, x1_buf, acc, w_sems, send_sems, recv_sems, x_sem, out_sems, *, layer, tiles, chunks):
    peer = 1 - lax.axis_index("tp")
    offs = [sum(tiles[:i]) for i in range(len(tiles))]
    starts = [sum(chunks[:i]) for i in range(len(chunks))]

    def w_copies(i):
        c = pl.ds(offs[i], tiles[i])
        return (
            pltpu.make_async_copy(wg_hbm.at[layer, :, c], wg.at[:, c], w_sems.at[i, 0]),
            pltpu.make_async_copy(wu_hbm.at[layer, :, c], wu.at[:, c], w_sems.at[i, 1]),
            pltpu.make_async_copy(wd_hbm.at[layer, c], wd.at[c], w_sems.at[i, 2]),
        )

    for i in range(len(tiles)):
        for copy in w_copies(i):
            copy.start()
    x_copy = pltpu.make_async_copy(x1_hbm, x1_buf, x_sem.at[0])
    x_copy.start()
    barrier = pltpu.get_barrier_semaphore()
    pl.semaphore_signal(barrier, inc=1, device_id={"tp": peer}, device_id_type=MESH)
    pl.semaphore_wait(barrier, 1)

    swaps = []
    for ci, n in enumerate(chunks):
        r = pl.ds(starts[ci], n)
        for i, t in enumerate(tiles):
            if ci == 0:
                for copy in w_copies(i):
                    copy.wait()
            c = pl.ds(offs[i], t)
            normed = h_ref[r, :]
            gate = jnp.dot(normed, wg[:, c], preferred_element_type=jnp.float32)
            up = jnp.dot(normed, wu[:, c], preferred_element_type=jnp.float32)
            act = (gate * jax.nn.sigmoid(gate) * up).astype(jnp.bfloat16)
            part = jnp.dot(act, wd[c, :], preferred_element_type=jnp.float32)
            if i == 0:
                acc[:n, :] = part
            elif i < len(tiles) - 1:
                acc[:n, :] += part
            else:
                send[r, :] = (acc[:n, :] + part).astype(jnp.bfloat16)
        swap = pltpu.make_async_remote_copy(src_ref=send.at[r], dst_ref=recv.at[r], send_sem=send_sems.at[ci], recv_sem=recv_sems.at[ci], device_id={"tp": peer}, device_id_type=MESH)
        swap.start()
        swaps.append(swap)

    x_copy.wait()
    out_copies = []
    for ci, n in enumerate(chunks):
        r = pl.ds(starts[ci], n)
        swaps[ci].wait()
        total = send[r, :].astype(jnp.float32) + recv[r, :].astype(jnp.float32)
        x1_buf[r, :] = (x1_buf[r, :].astype(jnp.float32) + total).astype(jnp.bfloat16)
        out_copy = pltpu.make_async_copy(x1_buf.at[r], out_hbm.at[r], out_sems.at[ci])
        out_copy.start()
        out_copies.append(out_copy)
    for out_copy in out_copies:
        out_copy.wait()


def mlp(layer, h2, x1, wg, wu, wd, cid):
    rows, width = h2.shape
    cols = wg.shape[2]
    tiles = (256, 512, 768, 1024, 1024, 896)
    chunks = (256,) * (rows // 256)
    nt, nc = len(tiles), len(chunks)
    anys = pl.BlockSpec(memory_space=pl.ANY)
    bf = jnp.bfloat16
    dma = pltpu.SemaphoreType.DMA
    return pl.pallas_call(
        functools.partial(mlp_kernel, layer=layer, tiles=tiles, chunks=chunks),
        in_specs=[pl.BlockSpec(memory_space=pltpu.VMEM), anys, anys, anys, anys],
        out_specs=anys,
        out_shape=jax.ShapeDtypeStruct((rows, width), bf),
        scratch_shapes=[
            pltpu.VMEM((width, cols), bf), pltpu.VMEM((width, cols), bf), pltpu.VMEM((cols, width), bf),
            pltpu.VMEM((rows, width), bf), pltpu.VMEM((rows, width), bf), pltpu.VMEM((rows, width), bf),
            pltpu.VMEM((max(chunks), width), jnp.float32),
            dma((nt, 3)), dma((nc,)), dma((nc,)), dma((1,)), dma((nc,)),
        ],
        compiler_params=pltpu.CompilerParams(vmem_limit_bytes=67043328, collective_id=cid, has_side_effects=True),
        cost_estimate=pl.CostEstimate(flops=6 * rows * width * cols, bytes_accessed=6 * width * cols, transcendentals=0),
        name="mlp",
    )(h2, x1, wg, wu, wd)


def solution(mesh):
    cp_size = mesh.shape["cp"]

    def local_step(x_in, positions, attn_gain, mlp_gain, w_query, b_query, w_key, b_key, w_value, b_value, w_out, w_gate, w_up, w_down):
        block_dev = x_in.shape[0]
        tp = lax.axis_index("tp")
        inv_freq = 1.0 / (1000000.0 ** (jnp.arange(0, HEAD_DIM, 2, dtype=jnp.float32) / HEAD_DIM))
        angles = positions.astype(jnp.float32)[:, None] * inv_freq[None, :]
        cos_half, sin_half = jnp.cos(angles), jnp.sin(angles)
        cos_tab = jnp.concatenate([cos_half, cos_half], axis=1)
        sin_tab = jnp.concatenate([-sin_half, sin_half], axis=1)
        row = lambda a: a[:, None, :]
        attn_gain, mlp_gain, b_query, b_key, b_value = (row(a) for a in (attn_gain, mlp_gain, b_query, b_key, b_value))

        place = jnp.reshape(tp, (1,)).astype(jnp.int32)
        hidden, w_peer, caches = x_in, None, []
        for layer, window_blocks in ((0, cp_size), (1, WINDOW // block_dev)):
            q, k, v, kv = qkv(layer, hidden, attn_gain, w_query, w_key, w_value, b_query, b_key, b_value, cos_tab, sin_tab)
            o, o_peer, *rest = attention(q, kv, w_out if layer == 0 else None, window_blocks, 512, 2 * layer)
            if layer == 0:
                w_peer = rest[0]
            x1, h2 = out_project(layer, place, o, o_peer, hidden, mlp_gain, w_out, w_peer)
            hidden = mlp(layer, h2, x1, w_gate, w_up, w_down, 2 * layer + 1)
            caches.append(k[:, None, :])
            caches.append(v[:, None, :])
        return hidden, caches[0], caches[1], caches[2], caches[3]

    weight_col = P(None, None, "tp")
    bias_col = P(None, "tp")
    weight_row = P(None, "tp", None)
    replicated = P(None, None)
    cache_spec = P("cp", "tp", None)
    in_specs = (P("cp", None), P("cp"), replicated, replicated, weight_col, bias_col, weight_col, bias_col, weight_col, bias_col, weight_row, weight_col, weight_col, weight_row)
    out_specs = (P("cp", None), cache_spec, cache_spec, cache_spec, cache_spec)
    return jax.shard_map(local_step, mesh=mesh, in_specs=in_specs, out_specs=out_specs, check_vma=False)
```

```python
import functools

import jax
import jax.numpy as jnp
from jax import lax
from jax.experimental import pallas as pl
from jax.experimental.pallas import tpu as pltpu
from jax.sharding import PartitionSpec as P

HEAD_DIM = 128
WINDOW = 4096
SCORE_SCALE = (HEAD_DIM ** -0.5) * 1.4426950408889634
MIB = 1024 * 1024
MESH = pl.DeviceIdType.MESH


def rms_rows(hidden_f, gain_f):
    variance = jnp.mean(hidden_f * hidden_f, axis=-1, keepdims=True)
    return (hidden_f * lax.rsqrt(variance + 1e-6) * gain_f).astype(jnp.bfloat16)


def qkv_kernel(x_ref, gain_ref, wq_ref, wk_ref, wv_ref, bq_ref, bk_ref, bv_ref, cos_ref, sin_ref, q_ref, k_ref, v_ref, kv_ref):
    normed = rms_rows(x_ref[...].astype(jnp.float32), gain_ref[...].astype(jnp.float32))
    cos_tab = cos_ref[...]
    sin_tab = sin_ref[...]

    def rope(block):
        return (block * cos_tab + pltpu.roll(block, HEAD_DIM // 2, 1) * sin_tab).astype(jnp.bfloat16)

    k_f = jnp.dot(normed, wk_ref[...], preferred_element_type=jnp.float32) + bk_ref[...].astype(jnp.float32)
    k_b = rope(k_f)
    k_ref[...] = k_b
    kv_ref[:, :HEAD_DIM] = k_b
    v_f = jnp.dot(normed, wv_ref[...], preferred_element_type=jnp.float32) + bv_ref[...].astype(jnp.float32)
    v_b = v_f.astype(jnp.bfloat16)
    v_ref[...] = v_b
    kv_ref[:, HEAD_DIM:] = v_b
    q_f = jnp.dot(normed, wq_ref[...], preferred_element_type=jnp.float32) + bq_ref[...].astype(jnp.float32)
    for head in range(q_ref.shape[1] // HEAD_DIM):
        cols = slice(head * HEAD_DIM, (head + 1) * HEAD_DIM)
        q_ref[:, cols] = rope(q_f[:, cols])


def qkv(layer, x, gain, wq, wk, wv, bq, bk, bv, cos_tab, sin_tab):
    rows, width = x.shape
    q_cols = wq.shape[2]
    block = min(rows, 256)

    def whole(w):
        return pl.BlockSpec((None,) + w.shape[1:], lambda i: (layer, 0, 0))

    def table():
        return pl.BlockSpec((block, HEAD_DIM), lambda i: (i, 0))

    def out(cols):
        return pl.BlockSpec((block, cols), lambda i: (i, 0))

    return pl.pallas_call(
        qkv_kernel,
        grid=(rows // block,),
        in_specs=[out(width)] + [whole(w) for w in (gain, wq, wk, wv, bq, bk, bv)] + [table(), table()],
        out_specs=[out(c) for c in (q_cols, HEAD_DIM, HEAD_DIM, 2 * HEAD_DIM)],
        out_shape=[jax.ShapeDtypeStruct((rows, c), jnp.bfloat16) for c in (q_cols, HEAD_DIM, HEAD_DIM, 2 * HEAD_DIM)],
        compiler_params=pltpu.CompilerParams(vmem_limit_bytes=32 * MIB),
        cost_estimate=pl.CostEstimate(flops=2 * rows * width * (q_cols + 256), bytes_accessed=rows * width * 4 + width * 2048, transcendentals=0),
        name="qkv",
    )(x, gain, wq, wk, wv, bq, bk, bv, cos_tab, sin_tab)


def attn_kernel(*refs, layer, bq, window_blocks):
    q_ref, kv_ref, w_out, o_ref, o_peer, w_peer, kv_buf, m_sc, l_sc, acc_sc, send_sems, recv_sems, o_send, o_recv, w_send, w_recv = refs
    rows = q_ref.shape[0]
    heads = q_ref.shape[1] // HEAD_DIM
    cp = lax.axis_index("cp")
    core, xpos, ypos = lax.rem(cp, 2), lax.rem(lax.div(cp, 2), 2), lax.div(cp, 4)
    to_mate, to_x, to_y = 1 - 2 * core, 2 - 4 * xpos, 4 - 8 * ypos
    mate, xnb, ynb, diag = cp + to_mate, cp + to_x, cp + to_y, cp + to_x + to_y
    half = rows // 2

    peer = 1 - lax.axis_index("tp")
    at_cp = lambda i: {"cp": i}
    whole = pl.ds(0, rows)

    def kv_copy(i, src, slot, part, dev):
        return pltpu.make_async_remote_copy(src_ref=src, dst_ref=kv_buf.at[slot, part], send_sem=send_sems.at[i], recv_sem=recv_sems.at[i], device_id=at_cp(dev), device_id_type=MESH)

    first, last = pl.ds(0, half), pl.ds(half, half)
    kv_copies = [
        kv_copy(0, kv_ref, cp, whole, mate),
        kv_copy(1, kv_ref, cp, whole, xnb),
        kv_copy(2, kv_ref, cp, whole, ynb),
        kv_copy(3, kv_buf.at[xnb], xnb, whole, mate),
        kv_copy(4, kv_buf.at[ynb], ynb, whole, mate),
        kv_copy(5, kv_buf.at[xnb, first], xnb, first, ynb),
        kv_copy(6, kv_buf.at[ynb, last], ynb, last, xnb),
        kv_copy(7, kv_buf.at[diag], diag, whole, mate),
    ]
    quarter = w_out.shape[1] // 2
    mine = pl.ds(pl.multiple_of(core * quarter, quarter), quarter)
    w_z = pltpu.make_async_remote_copy(src_ref=w_out.at[layer, mine], dst_ref=w_peer.at[mine], send_sem=w_send.at[0], recv_sem=w_recv.at[0], device_id={"tp": peer}, device_id_type=MESH)
    w_d = pltpu.make_async_remote_copy(src_ref=w_peer.at[mine], dst_ref=w_peer.at[mine], send_sem=w_send.at[1], recv_sem=w_recv.at[1], device_id=at_cp(mate), device_id_type=MESH)

    barrier = pltpu.get_barrier_semaphore()
    for dev in (at_cp(mate), at_cp(xnb), at_cp(ynb), {"tp": peer}):
        pl.semaphore_signal(barrier, inc=1, device_id=dev, device_id_type=MESH)
    pl.semaphore_wait(barrier, 4)
    for copy in kv_copies[:3]:
        copy.start()
    w_z.start()

    def o_copy(qb):
        part = pl.ds(pl.multiple_of(qb * bq, bq), bq)
        return pltpu.make_async_remote_copy(src_ref=o_ref.at[part], dst_ref=o_peer.at[part], send_sem=o_send.at[qb], recv_sem=o_recv.at[qb], device_id={"tp": peer}, device_id_type=MESH)

    def block(q0, kb, vb, keep):
        bk = kb.shape[0]

        def scores(h):
            qh = q_ref[pl.ds(q0, bq), h * HEAD_DIM:(h + 1) * HEAD_DIM]
            return lax.dot_general(qh, kb, (((1,), (1,)), ((), ())), preferred_element_type=jnp.float32)

        def soft(h, s):
            if keep is not None:
                s = jnp.where(keep, s, -1e30)
            m_old = m_sc[h]
            m_new = jnp.maximum(m_old, jnp.max(s, axis=1, keepdims=True) * SCORE_SCALE)
            m_sc[h] = m_new
            alpha = jnp.exp2(m_old - m_new)
            p = jnp.exp2(s * SCORE_SCALE - jnp.tile(m_new, (1, bk // HEAD_DIM)))
            if keep is not None:
                p = jnp.where(keep, p, 0.0)
            parts = [p[:, j:j + HEAD_DIM] for j in range(0, bk, HEAD_DIM)]
            while len(parts) > 1:
                parts = [parts[i] + parts[i + 1] for i in range(0, len(parts), 2)]
            l_sc[h] = l_sc[h] * alpha + parts[0]
            return p.astype(jnp.bfloat16), alpha

        def weigh(h, p, alpha):
            acc_sc[h] = acc_sc[h] * alpha + jnp.dot(p, vb, preferred_element_type=jnp.float32)

        s_of, p_of = {}, {}
        for i in range(heads + 2):
            if i < heads:
                s_of[i] = scores(i)
            if i >= 2:
                weigh(i - 2, *p_of.pop(i - 2))
            if 1 <= i <= heads:
                p_of[i - 1] = soft(i - 1, s_of.pop(i - 1))

    def split(ref, *at):
        return ref[at + (slice(None, HEAD_DIM),)], ref[at + (slice(HEAD_DIM, None),)]

    def q_block(qb, carry):
        q0 = pl.multiple_of(qb * bq, bq)
        m_sc[...] = jnp.full(m_sc.shape, -1e30, jnp.float32)
        l_sc[...] = jnp.zeros(l_sc.shape, jnp.float32)
        acc_sc[...] = jnp.zeros(acc_sc.shape, jnp.float32)
        row = lax.broadcasted_iota(jnp.int32, (bq, bq), 0)
        col = lax.broadcasted_iota(jnp.int32, (bq, bq), 1)

        def own_part(j, c):
            block(q0, *split(kv_ref, pl.ds(pl.multiple_of(j * bq, bq), bq)), None)
            return c

        block(q0, *split(kv_ref, pl.ds(q0, bq)), col <= row)
        lax.fori_loop(0, qb, own_part, 0)

        def step_body(step, c):
            src = cp + lax.rem(step, 2) * to_mate + lax.rem(lax.div(step, 2), 2) * to_x + lax.div(step, 4) * to_y
            @pl.when(qb == 0)
            def _():
                @pl.when(step == 1)
                def _():
                    kv_copies[0].wait_recv()

                @pl.when(step == 2)
                def _():
                    kv_copies[1].wait_recv()
                    kv_copies[3].start()
                    kv_copies[5].start()
                    kv_copies[2].wait_recv()
                    kv_copies[4].start()
                    kv_copies[6].start()

                @pl.when(step == 3)
                def _():
                    kv_copies[3].wait_recv()

                @pl.when(step == 5)
                def _():
                    kv_copies[4].wait_recv()

                @pl.when(step == 6)
                def _():
                    kv_copies[5].wait_recv()
                    kv_copies[6].wait_recv()
                    kv_copies[7].start()

                @pl.when(step == 7)
                def _():
                    kv_copies[7].wait_recv()
            @pl.when((src < cp) & (src > cp - window_blocks))
            def _():
                block(q0, *split(kv_buf, src, slice(None)), None)

            if window_blocks < 8:
                @pl.when(src == cp - window_blocks)
                def _():
                    block(q0, *split(kv_buf, src, pl.ds(q0, bq)), col > row)

                    def edge_part(j, cc):
                        block(q0, *split(kv_buf, src, pl.ds(pl.multiple_of(j * bq, bq), bq)), None)
                        return cc

                    lax.fori_loop(qb + 1, rows // bq, edge_part, 0)
            return c

        lax.fori_loop(1, 8, step_body, 0)
        for h in range(heads):
            total = jnp.sum(l_sc[h], axis=1, keepdims=True)
            o_ref[pl.ds(q0, bq), h * HEAD_DIM:(h + 1) * HEAD_DIM] = (acc_sc[h] / total).astype(jnp.bfloat16)
        @pl.when(qb < rows // bq - 1)
        def _():
            o_copy(qb).start()

        @pl.when(qb == 0)
        def _():
            w_z.wait_recv()
            w_d.start()
        return carry

    lax.fori_loop(0, rows // bq, q_block, 0)
    for copy in kv_copies:
        copy.wait_send()
    w_z.wait_send()
    w_d.wait()
    for qb in range(rows // bq - 1):
        o_copy(qb).wait()

def attention(layer, q, kv, w_out, window_blocks, bq, cid):
    rows, cols = q.shape
    heads = cols // HEAD_DIM
    bf = jnp.bfloat16
    vm = pl.BlockSpec(memory_space=pltpu.VMEM)
    anys = pl.BlockSpec(memory_space=pl.ANY)
    nq = rows // bq
    outs = [jax.ShapeDtypeStruct(sh, bf) for sh in ((rows, cols), (rows - bq, cols), w_out.shape[1:])]
    dma = pltpu.SemaphoreType.DMA
    return pl.pallas_call(
        functools.partial(attn_kernel, layer=layer, bq=bq, window_blocks=window_blocks),
        in_specs=[vm, vm, anys],
        out_specs=[vm, anys, anys],
        out_shape=outs,
        scratch_shapes=[pltpu.VMEM((8, rows, 2 * HEAD_DIM), bf)] + [pltpu.VMEM((heads, bq, HEAD_DIM), jnp.float32)] * 3
        + [dma((8,)), dma((8,)), dma((nq,)), dma((nq,)), dma((2,)), dma((2,))],
        compiler_params=pltpu.CompilerParams(vmem_limit_bytes=48 * MIB, collective_id=cid, has_side_effects=True),
        cost_estimate=pl.CostEstimate(flops=16 * rows * rows * cols, bytes_accessed=rows * cols * 6, transcendentals=0),
        name="attn",
    )(q, kv, w_out)


def tail_kernel(*refs, layer, tiles, chunks, head_rows, with_qkv):
    refs = list(refs)
    o_own, o_head, x_hbm, gain_ref, w_out, w_peer, wg_hbm, wu_hbm, wd_hbm = refs[:9]
    refs = refs[9:]
    if with_qkv:
        again_ref, wq_hbm, wk_hbm, wv_hbm, bq_ref, bk_ref, bv_ref, cos_hbm, sin_hbm = refs[:9]
        refs = refs[9:]
    out_hbm = refs.pop(0)
    if with_qkv:
        q_hbm, k_hbm, v_hbm, kv_hbm = refs[:4]
        refs = refs[4:]
    w_full, o_full, hs, recv, xbuf, acc, wg, wu, wd, w_sems, in_sems, x_sems, o_sems, send_sems, recv_sems, out_sems, qkv_sems = refs
    rows, half = o_own.shape
    tp = lax.axis_index("tp")
    peer = {"tp": 1 - tp}
    own_cols = pl.ds(pl.multiple_of(tp * half, half), half)
    peer_cols = pl.ds(pl.multiple_of((1 - tp) * half, half), half)
    head_part, tail_part = pl.ds(0, head_rows), pl.ds(head_rows, rows - head_rows)
    offs = [sum(tiles[:i]) for i in range(len(tiles))]
    starts = [sum(chunks[:i]) for i in range(len(chunks))]

    def w_copies(i):
        c = pl.ds(offs[i], tiles[i])
        return (
            pltpu.make_async_copy(wg_hbm.at[layer, :, c], wg.at[:, c], w_sems.at[i, 0]),
            pltpu.make_async_copy(wu_hbm.at[layer, :, c], wu.at[:, c], w_sems.at[i, 1]),
            pltpu.make_async_copy(wd_hbm.at[layer, c], wd.at[c], w_sems.at[i, 2]),
        )

    def x_copy(ci):
        n = chunks[ci]
        return pltpu.make_async_copy(x_hbm.at[pl.ds(starts[ci], n)], xbuf.at[ci % 2, pl.ds(0, n)], x_sems.at[ci])

    first = [
        pltpu.make_async_copy(w_out.at[layer], w_full.at[own_cols], in_sems.at[0]),
        pltpu.make_async_copy(w_peer, w_full.at[peer_cols], in_sems.at[1]),
        pltpu.make_async_copy(o_own, o_full.at[:, own_cols], in_sems.at[2]),
        pltpu.make_async_copy(o_head, o_full.at[head_part, peer_cols], in_sems.at[3]),
        x_copy(0),
    ]
    for copy in first:
        copy.start()
    barrier = pltpu.get_barrier_semaphore()
    pl.semaphore_signal(barrier, inc=1, device_id=peer, device_id_type=MESH)
    pl.semaphore_wait(barrier, 1)
    o_swap = pltpu.make_async_remote_copy(src_ref=o_own.at[tail_part], dst_ref=o_full.at[tail_part, own_cols], send_sem=o_sems.at[0], recv_sem=o_sems.at[1], device_id=peer, device_id_type=MESH)
    o_swap.start()
    for i in range(len(tiles)):
        for copy in w_copies(i):
            copy.start()
    for copy in first:
        copy.wait()

    swaps = []
    tail_here = False
    for ci, n in enumerate(chunks):
        r = pl.ds(starts[ci], n)
        if starts[ci] + n > head_rows and not tail_here:
            o_swap.wait()
            tail_here = True
        if ci > 0:
            x_copy(ci).wait()
        if ci + 1 < len(chunks):
            x_copy(ci + 1).start()
        prod = jnp.dot(o_full[r, :], w_full[...], preferred_element_type=jnp.float32)
        x1 = (xbuf[ci % 2, pl.ds(0, n), :].astype(jnp.float32) + prod).astype(jnp.bfloat16)
        o_full[r, :] = x1
        hs[r, :] = rms_rows(x1.astype(jnp.float32), gain_ref[...].astype(jnp.float32))
        for i, t in enumerate(tiles):
            if ci == 0:
                for copy in w_copies(i):
                    copy.wait()
            c = pl.ds(offs[i], t)
            normed = hs[r, :]
            gate = jnp.dot(normed, wg[:, c], preferred_element_type=jnp.float32)
            up = jnp.dot(normed, wu[:, c], preferred_element_type=jnp.float32)
            act = (gate * jax.nn.sigmoid(gate) * up).astype(jnp.bfloat16)
            part = jnp.dot(act, wd[c, :], preferred_element_type=jnp.float32)
            if i == 0:
                acc[:n, :] = part
            elif i < len(tiles) - 1:
                acc[:n, :] += part
            else:
                hs[r, :] = (acc[:n, :] + part).astype(jnp.bfloat16)
        swap = pltpu.make_async_remote_copy(src_ref=hs.at[r], dst_ref=recv.at[r], send_sem=send_sems.at[ci], recv_sem=recv_sems.at[ci], device_id=peer, device_id_type=MESH)
        swap.start()
        swaps.append(swap)

    waits = []
    if with_qkv:
        q_cols = wq_hbm.shape[2]
        kv_cols = q_cols + 2 * HEAD_DIM
        nxt = layer + 1
        loads = [
            pltpu.make_async_copy(wq_hbm.at[nxt], w_full.at[:, pl.ds(0, q_cols)], qkv_sems.at[0]),
            pltpu.make_async_copy(wk_hbm.at[nxt], w_full.at[:, pl.ds(q_cols, HEAD_DIM)], qkv_sems.at[1]),
            pltpu.make_async_copy(wv_hbm.at[nxt], w_full.at[:, pl.ds(q_cols + HEAD_DIM, HEAD_DIM)], qkv_sems.at[2]),
        ]
        for ci, n in enumerate(chunks):
            r = pl.ds(starts[ci], n)
            at = ci * 2 * HEAD_DIM
            loads.append(pltpu.make_async_copy(cos_hbm.at[r], acc.at[pl.ds(0, n), pl.ds(at, HEAD_DIM)], qkv_sems.at[3 + 2 * ci]))
            loads.append(pltpu.make_async_copy(sin_hbm.at[r], acc.at[pl.ds(0, n), pl.ds(at + HEAD_DIM, HEAD_DIM)], qkv_sems.at[4 + 2 * ci]))
        for copy in loads:
            copy.start()
        for copy in loads:
            copy.wait()
    for ci, n in enumerate(chunks):
        r = pl.ds(starts[ci], n)
        swaps[ci].wait()
        total = hs[r, :].astype(jnp.float32) + recv[r, :].astype(jnp.float32)
        x2 = (o_full[r, :].astype(jnp.float32) + total).astype(jnp.bfloat16)
        o_full[r, :] = x2
        done = [pltpu.make_async_copy(o_full.at[r], out_hbm.at[r], out_sems.at[ci, 0])]
        if with_qkv:
            at = ci * 2 * HEAD_DIM
            cos_tab = acc[:n, at:at + HEAD_DIM]
            sin_tab = acc[:n, at + HEAD_DIM:at + 2 * HEAD_DIM]
            normed = rms_rows(x2.astype(jnp.float32), again_ref[...].astype(jnp.float32))
            proj = jnp.dot(normed, w_full[:, :kv_cols], preferred_element_type=jnp.float32)

            def rope(cols, bias):
                block = proj[:, cols] + bias
                return (block * cos_tab + pltpu.roll(block, HEAD_DIM // 2, 1) * sin_tab).astype(jnp.bfloat16)

            for at in range(0, q_cols, HEAD_DIM):
                cols = slice(at, at + HEAD_DIM)
                hs[r, cols] = rope(cols, bq_ref[:, cols].astype(jnp.float32))
            k_cols, v_cols = slice(q_cols, q_cols + HEAD_DIM), slice(q_cols + HEAD_DIM, kv_cols)
            hs[r, k_cols] = rope(k_cols, bk_ref[...].astype(jnp.float32))
            hs[r, v_cols] = (proj[:, v_cols] + bv_ref[...].astype(jnp.float32)).astype(jnp.bfloat16)
            done.append(pltpu.make_async_copy(hs.at[r, pl.ds(0, q_cols)], q_hbm.at[r], out_sems.at[ci, 1]))
            done.append(pltpu.make_async_copy(hs.at[r, pl.ds(q_cols, HEAD_DIM)], k_hbm.at[r], out_sems.at[ci, 2]))
            done.append(pltpu.make_async_copy(hs.at[r, pl.ds(q_cols + HEAD_DIM, HEAD_DIM)], v_hbm.at[r], out_sems.at[ci, 3]))
            done.append(pltpu.make_async_copy(hs.at[r, pl.ds(q_cols, 2 * HEAD_DIM)], kv_hbm.at[r], out_sems.at[ci, 4]))
        for copy in done:
            copy.start()
        waits += done
    for copy in waits:
        copy.wait()


def layer_tail(layer, o_own, o_head, x, gain, w_out, w_peer, wg, wu, wd, next_qkv, cid):
    rows, half = o_own.shape
    width = x.shape[1]
    cols = wg.shape[2]
    tiles = (256, 512, 768, 768, 768, 768, 640)
    chunks = (256,) * (rows // 256)
    nt, nc = len(tiles), len(chunks)
    anys = pl.BlockSpec(memory_space=pl.ANY)
    bf = jnp.bfloat16
    dma = pltpu.SemaphoreType.DMA

    def layer_row(a, l):
        return pl.BlockSpec((None,) + a.shape[1:], lambda i: (l, 0, 0))

    args = [o_own, o_head, x, gain, w_out, w_peer, wg, wu, wd]
    specs = [anys] * 3 + [layer_row(gain, layer)] + [anys] * 5
    outs = [jax.ShapeDtypeStruct((rows, width), bf)]
    if next_qkv is not None:
        again, wq, wk, wv, bq, bk, bv, cos_tab, sin_tab = next_qkv
        args += list(next_qkv)
        specs += [layer_row(again, layer + 1)] + [anys] * 3 + [layer_row(b, layer + 1) for b in (bq, bk, bv)] + [anys] * 2
        outs += [jax.ShapeDtypeStruct((rows, c), bf) for c in (wq.shape[2], HEAD_DIM, HEAD_DIM, 2 * HEAD_DIM)]
    return pl.pallas_call(
        functools.partial(tail_kernel, layer=layer, tiles=tiles, chunks=chunks, head_rows=o_head.shape[0], with_qkv=next_qkv is not None),
        grid=(1,),
        in_specs=specs,
        out_specs=[anys] * len(outs),
        out_shape=outs,
        scratch_shapes=[
            pltpu.VMEM((2 * half, width), bf), pltpu.VMEM((rows, width), bf), pltpu.VMEM((rows, width), bf), pltpu.VMEM((rows, width), bf),
            pltpu.VMEM((2, max(chunks), width), bf), pltpu.VMEM((max(chunks), width), jnp.float32),
            pltpu.VMEM((width, cols), bf), pltpu.VMEM((width, cols), bf), pltpu.VMEM((cols, width), bf),
            dma((nt, 3)), dma((4,)), dma((nc,)), dma((2,)), dma((nc,)), dma((nc,)), dma((nc, 5)), dma((3 + 2 * nc,)),
        ],
        compiler_params=pltpu.CompilerParams(vmem_limit_bytes=67043328, collective_id=cid, has_side_effects=True),
        cost_estimate=pl.CostEstimate(flops=6 * rows * width * cols, bytes_accessed=6 * width * cols, transcendentals=0),
        name="tail",
    )(*args)


def solution(mesh):
    cp_size = mesh.shape["cp"]

    def local_step(x_in, positions, attn_gain, mlp_gain, w_query, b_query, w_key, b_key, w_value, b_value, w_out, w_gate, w_up, w_down):
        block_dev = x_in.shape[0]
        inv_freq = 1.0 / (1000000.0 ** (jnp.arange(0, HEAD_DIM, 2, dtype=jnp.float32) / HEAD_DIM))
        angles = positions.astype(jnp.float32)[:, None] * inv_freq[None, :]
        cos_half, sin_half = jnp.cos(angles), jnp.sin(angles)
        cos_tab = jnp.concatenate([cos_half, cos_half], axis=1)
        sin_tab = jnp.concatenate([-sin_half, sin_half], axis=1)
        row = lambda a: a[:, None, :]
        attn_gain, mlp_gain, b_query, b_key, b_value = (row(a) for a in (attn_gain, mlp_gain, b_query, b_key, b_value))

        qkv_args = (attn_gain, w_query, w_key, w_value, b_query, b_key, b_value, cos_tab, sin_tab)
        hidden, caches = x_in, []
        q, k, v, kv = qkv(0, hidden, *qkv_args)
        for layer, window_blocks in ((0, cp_size), (1, WINDOW // block_dev)):
            caches.append(k[:, None, :])
            caches.append(v[:, None, :])
            o, o_head, w_peer = attention(layer, q, kv, w_out, window_blocks, 512, 2 * layer)
            hidden, *rest = layer_tail(layer, o, o_head, hidden, mlp_gain, w_out, w_peer, w_gate, w_up, w_down, qkv_args if layer == 0 else None, 2 * layer + 1)
            if layer == 0:
                q, k, v, kv = rest
        return hidden, caches[0], caches[1], caches[2], caches[3]

    weight_col = P(None, None, "tp")
    bias_col = P(None, "tp")
    weight_row = P(None, "tp", None)
    replicated = P(None, None)
    cache_spec = P("cp", "tp", None)
    in_specs = (P("cp", None), P("cp"), replicated, replicated, weight_col, bias_col, weight_col, bias_col, weight_col, bias_col, weight_row, weight_col, weight_col, weight_row)
    out_specs = (P("cp", None), cache_spec, cache_spec, cache_spec, cache_spec)
    return jax.shard_map(local_step, mesh=mesh, in_specs=in_specs, out_specs=out_specs, check_vma=False)
```

```python
import functools

import jax
import jax.numpy as jnp
from jax import lax
from jax.experimental import pallas as pl
from jax.experimental.pallas import tpu as pltpu
from jax.sharding import PartitionSpec as P

HEAD_DIM = 128
WINDOW = 4096
SCORE_SCALE = (HEAD_DIM ** -0.5) * 1.4426950408889634
MIB = 1024 * 1024
MESH = pl.DeviceIdType.MESH


def rms_rows(hidden_f, gain_f):
    variance = jnp.mean(hidden_f * hidden_f, axis=-1, keepdims=True)
    return (hidden_f * lax.rsqrt(variance + 1e-6) * gain_f).astype(jnp.bfloat16)


def qkv_kernel(x_hbm, gain_ref, wq_hbm, wk_hbm, wv_hbm, bq_ref, bk_ref, bv_ref, cos_ref, sin_ref, q_ref, k_hbm, v_hbm, kv_ref, x_buf, w_buf, w_sems, x_sems, kv_sems, *, chunks):
    q_cols = wq_hbm.shape[2]
    k_cols, v_cols = slice(q_cols, q_cols + HEAD_DIM), slice(q_cols + HEAD_DIM, q_cols + 2 * HEAD_DIM)
    loads = [
        pltpu.make_async_copy(wq_hbm.at[0], w_buf.at[:, pl.ds(0, q_cols)], w_sems.at[0]),
        pltpu.make_async_copy(wk_hbm.at[0], w_buf.at[:, pl.ds(q_cols, HEAD_DIM)], w_sems.at[1]),
        pltpu.make_async_copy(wv_hbm.at[0], w_buf.at[:, pl.ds(q_cols + HEAD_DIM, HEAD_DIM)], w_sems.at[2]),
    ]
    rows = x_hbm.shape[0] // chunks

    def part(i):
        return pl.ds(pl.multiple_of(i * rows, rows), rows)

    def x_load(i):
        return pltpu.make_async_copy(x_hbm.at[part(i)], x_buf.at[part(i)], x_sems.at[i])

    x_load(0).start()
    for copy in loads:
        copy.start()
    for i in range(1, chunks):
        x_load(i).start()
    gain = gain_ref[...].astype(jnp.float32)[:1]
    b_q, b_k, b_v = (b[...].astype(jnp.float32)[:1] for b in (bq_ref, bk_ref, bv_ref))

    def run_part(i, carry):
        r = part(i)
        x_load(i).wait()
        normed = rms_rows(x_buf[r, :].astype(jnp.float32), gain)

        @pl.when(i == 0)
        def _():
            for copy in loads:
                copy.wait()

        proj = jnp.dot(normed, w_buf[...], preferred_element_type=jnp.float32)
        cos_tab, sin_tab = cos_ref[r, :], sin_ref[r, :]

        def rope(cols, bias):
            block = proj[:, cols] + bias
            return (block * cos_tab + pltpu.roll(block, HEAD_DIM // 2, 1) * sin_tab).astype(jnp.bfloat16)

        for at in range(0, q_cols, HEAD_DIM):
            cols = slice(at, at + HEAD_DIM)
            q_ref[r, cols] = rope(cols, b_q[:, cols])
        kv_ref[r, :HEAD_DIM] = rope(k_cols, b_k)
        kv_ref[r, HEAD_DIM:] = (proj[:, v_cols] + b_v).astype(jnp.bfloat16)
        return carry

    lax.fori_loop(0, chunks, run_part, 0)
    stores = [
        pltpu.make_async_copy(kv_ref.at[:, pl.ds(0, HEAD_DIM)], k_hbm, kv_sems.at[0]),
        pltpu.make_async_copy(kv_ref.at[:, pl.ds(HEAD_DIM, HEAD_DIM)], v_hbm, kv_sems.at[1]),
    ]
    for copy in stores:
        copy.start()
    for copy in stores:
        copy.wait()


def qkv(x, gain, wq, wk, wv, bq, bk, bv, cos_tab, sin_tab):
    rows, width = x.shape
    q_cols = wq.shape[2]
    chunks = 4
    vm = pl.BlockSpec(memory_space=pltpu.VMEM)
    hbm = pl.BlockSpec(memory_space=pltpu.HBM)
    anys = pl.BlockSpec(memory_space=pl.ANY)
    dma = pltpu.SemaphoreType.DMA
    return pl.pallas_call(
        functools.partial(qkv_kernel, chunks=chunks),
        in_specs=[anys, vm, anys, anys, anys] + [vm] * 5,
        out_specs=[vm, hbm, hbm, vm],
        out_shape=[jax.ShapeDtypeStruct((rows, c), jnp.bfloat16) for c in (q_cols, HEAD_DIM, HEAD_DIM, 2 * HEAD_DIM)],
        scratch_shapes=[pltpu.VMEM((rows, width), jnp.bfloat16), pltpu.VMEM((width, q_cols + 2 * HEAD_DIM), jnp.bfloat16), dma((3,)), dma((chunks,)), dma((2,))],
        compiler_params=pltpu.CompilerParams(vmem_limit_bytes=48 * MIB),
        cost_estimate=pl.CostEstimate(flops=2 * rows * width * (q_cols + 256), bytes_accessed=rows * width * 4 + width * 2048, transcendentals=0),
        name="qkv",
    )(x, gain, wq, wk, wv, bq, bk, bv, cos_tab, sin_tab)


def attn_kernel(*refs, layer, bq, window_blocks):
    q_ref, kv_ref, w_out, o_hbm, o_peer, w_peer, kv_buf, o_ref, m_sc, l_sc, acc_sc, send_sems, recv_sems, o_send, o_recv, o_out, w_send, w_recv = refs
    rows = q_ref.shape[0]
    heads = q_ref.shape[1] // HEAD_DIM
    cp = lax.axis_index("cp")
    core, xpos, ypos = lax.rem(cp, 2), lax.rem(lax.div(cp, 2), 2), lax.div(cp, 4)
    to_mate, to_x, to_y = 1 - 2 * core, 2 - 4 * xpos, 4 - 8 * ypos
    mate, xnb, ynb, diag = cp + to_mate, cp + to_x, cp + to_y, cp + to_x + to_y
    half = rows // 2

    peer = 1 - lax.axis_index("tp")
    at_cp = lambda i: {"cp": i}
    whole = pl.ds(0, rows)

    def kv_copy(i, src, slot, part, dev):
        return pltpu.make_async_remote_copy(src_ref=src, dst_ref=kv_buf.at[slot, part], send_sem=send_sems.at[i], recv_sem=recv_sems.at[i], device_id=at_cp(dev), device_id_type=MESH)

    first, last = pl.ds(0, half), pl.ds(half, half)
    kv_copies = [
        kv_copy(0, kv_ref, cp, whole, mate),
        kv_copy(1, kv_ref, cp, whole, xnb),
        kv_copy(2, kv_ref, cp, whole, ynb),
        kv_copy(3, kv_buf.at[xnb], xnb, whole, mate),
        kv_copy(4, kv_buf.at[ynb], ynb, whole, mate),
        kv_copy(5, kv_buf.at[xnb, first], xnb, first, ynb),
        kv_copy(6, kv_buf.at[ynb, last], ynb, last, xnb),
        kv_copy(7, kv_buf.at[diag], diag, whole, mate),
    ]
    quarter = w_out.shape[1] // 2
    mine = pl.ds(pl.multiple_of(core * quarter, quarter), quarter)
    w_z = pltpu.make_async_remote_copy(src_ref=w_out.at[layer, mine], dst_ref=w_peer.at[mine], send_sem=w_send.at[0], recv_sem=w_recv.at[0], device_id={"tp": peer}, device_id_type=MESH)
    w_d = pltpu.make_async_remote_copy(src_ref=w_peer.at[mine], dst_ref=w_peer.at[mine], send_sem=w_send.at[1], recv_sem=w_recv.at[1], device_id=at_cp(mate), device_id_type=MESH)

    barrier = pltpu.get_barrier_semaphore()
    for dev in (at_cp(mate), at_cp(xnb), at_cp(ynb), {"tp": peer}):
        pl.semaphore_signal(barrier, inc=1, device_id=dev, device_id_type=MESH)
    pl.semaphore_wait(barrier, 4)
    for copy in kv_copies[:3]:
        copy.start()
    w_z.start()

    def o_copy(qb):
        part = pl.ds(pl.multiple_of(qb * bq, bq), bq)
        return pltpu.make_async_remote_copy(src_ref=o_ref.at[part], dst_ref=o_peer.at[part], send_sem=o_send.at[qb], recv_sem=o_recv.at[qb], device_id={"tp": peer}, device_id_type=MESH)

    def o_store(qb):
        part = pl.ds(pl.multiple_of(qb * bq, bq), bq)
        return pltpu.make_async_copy(o_ref.at[part], o_hbm.at[part], o_out.at[qb])

    def block(q0, kb, vb, keep):
        bk = kb.shape[0]

        def scores(h):
            qh = q_ref[pl.ds(q0, bq), h * HEAD_DIM:(h + 1) * HEAD_DIM]
            return lax.dot_general(qh, kb, (((1,), (1,)), ((), ())), preferred_element_type=jnp.float32)

        def soft(h, s):
            if keep is not None:
                s = jnp.where(keep, s, -1e30)
            m_old = m_sc[h]
            m_new = jnp.maximum(m_old, jnp.max(s, axis=1, keepdims=True) * SCORE_SCALE)
            m_sc[h] = m_new
            alpha = jnp.exp2(m_old - m_new)
            p = jnp.exp2(s * SCORE_SCALE - jnp.tile(m_new, (1, bk // HEAD_DIM)))
            if keep is not None:
                p = jnp.where(keep, p, 0.0)
            parts = [p[:, j:j + HEAD_DIM] for j in range(0, bk, HEAD_DIM)]
            while len(parts) > 1:
                parts = [parts[i] + parts[i + 1] for i in range(0, len(parts), 2)]
            l_sc[h] = l_sc[h] * alpha + parts[0]
            return p.astype(jnp.bfloat16), alpha

        def weigh(h, p, alpha):
            acc_sc[h] = acc_sc[h] * alpha + jnp.dot(p, vb, preferred_element_type=jnp.float32)

        s_of, p_of = {}, {}
        for i in range(heads + 2):
            if i < heads:
                s_of[i] = scores(i)
            if i >= 2:
                weigh(i - 2, *p_of.pop(i - 2))
            if 1 <= i <= heads:
                p_of[i - 1] = soft(i - 1, s_of.pop(i - 1))

    def split(ref, *at):
        return ref[at + (slice(None, HEAD_DIM),)], ref[at + (slice(HEAD_DIM, None),)]

    def q_block(qb, carry):
        q0 = pl.multiple_of(qb * bq, bq)
        m_sc[...] = jnp.full(m_sc.shape, -1e30, jnp.float32)
        l_sc[...] = jnp.zeros(l_sc.shape, jnp.float32)
        acc_sc[...] = jnp.zeros(acc_sc.shape, jnp.float32)
        row = lax.broadcasted_iota(jnp.int32, (bq, bq), 0)
        col = lax.broadcasted_iota(jnp.int32, (bq, bq), 1)

        def own_part(j, c):
            block(q0, *split(kv_ref, pl.ds(pl.multiple_of(j * bq, bq), bq)), None)
            return c

        block(q0, *split(kv_ref, pl.ds(q0, bq)), col <= row)
        lax.fori_loop(0, qb, own_part, 0)

        def step_body(step, c):
            src = cp + lax.rem(step, 2) * to_mate + lax.rem(lax.div(step, 2), 2) * to_x + lax.div(step, 4) * to_y
            @pl.when(qb == 0)
            def _():
                @pl.when(step == 1)
                def _():
                    kv_copies[0].wait_recv()

                @pl.when(step == 2)
                def _():
                    kv_copies[1].wait_recv()
                    kv_copies[3].start()
                    kv_copies[5].start()
                    kv_copies[2].wait_recv()
                    kv_copies[4].start()
                    kv_copies[6].start()

                @pl.when(step == 3)
                def _():
                    kv_copies[3].wait_recv()

                @pl.when(step == 5)
                def _():
                    kv_copies[4].wait_recv()

                @pl.when(step == 6)
                def _():
                    kv_copies[5].wait_recv()
                    kv_copies[6].wait_recv()
                    kv_copies[7].start()

                @pl.when(step == 7)
                def _():
                    kv_copies[7].wait_recv()
            @pl.when((src < cp) & (src > cp - window_blocks))
            def _():
                block(q0, *split(kv_buf, src, slice(None)), None)

            if window_blocks < 8:
                @pl.when(src == cp - window_blocks)
                def _():
                    block(q0, *split(kv_buf, src, pl.ds(q0, bq)), col > row)

                    def edge_part(j, cc):
                        block(q0, *split(kv_buf, src, pl.ds(pl.multiple_of(j * bq, bq), bq)), None)
                        return cc

                    lax.fori_loop(qb + 1, rows // bq, edge_part, 0)
            return c

        lax.fori_loop(1, 8, step_body, 0)
        for h in range(heads):
            total = jnp.sum(l_sc[h], axis=1, keepdims=True)
            o_ref[pl.ds(q0, bq), h * HEAD_DIM:(h + 1) * HEAD_DIM] = (acc_sc[h] / total).astype(jnp.bfloat16)
        o_store(qb).start()

        @pl.when(qb < rows // bq - 1)
        def _():
            o_copy(qb).start()

        @pl.when(qb == 0)
        def _():
            w_z.wait_recv()
            w_d.start()
        return carry

    lax.fori_loop(0, rows // bq, q_block, 0)
    for copy in kv_copies:
        copy.wait_send()
    w_z.wait_send()
    w_d.wait()
    for qb in range(rows // bq):
        o_store(qb).wait()
    for qb in range(rows // bq - 1):
        o_copy(qb).wait()

def attention(layer, q, kv, w_out, window_blocks, bq, cid):
    rows, cols = q.shape
    heads = cols // HEAD_DIM
    bf = jnp.bfloat16
    vm = pl.BlockSpec(memory_space=pltpu.VMEM)
    anys = pl.BlockSpec(memory_space=pl.ANY)
    nq = rows // bq
    outs = [jax.ShapeDtypeStruct(sh, bf) for sh in ((rows, cols), (rows - bq, cols), w_out.shape[1:])]
    dma = pltpu.SemaphoreType.DMA
    return pl.pallas_call(
        functools.partial(attn_kernel, layer=layer, bq=bq, window_blocks=window_blocks),
        in_specs=[vm, vm, anys],
        out_specs=[pl.BlockSpec(memory_space=pltpu.HBM)] * 3,
        out_shape=outs,
        scratch_shapes=[pltpu.VMEM((8, rows, 2 * HEAD_DIM), bf), pltpu.VMEM((rows, cols), bf)] + [pltpu.VMEM((heads, bq, HEAD_DIM), jnp.float32)] * 3
        + [dma((8,)), dma((8,)), dma((nq,)), dma((nq,)), dma((nq,)), dma((2,)), dma((2,))],
        compiler_params=pltpu.CompilerParams(vmem_limit_bytes=67043328, collective_id=cid, has_side_effects=True),
        cost_estimate=pl.CostEstimate(flops=16 * rows * rows * cols, bytes_accessed=rows * cols * 6, transcendentals=0),
        name="attn",
    )(q, kv, w_out)


def tail_kernel(*refs, layer, tile, chunk, head_rows, with_qkv):
    refs = list(refs)
    o_own, o_head, x_hbm, gain_ref, w_out, w_peer, wg_hbm, wu_hbm, wd_hbm = refs[:9]
    refs = refs[9:]
    if with_qkv:
        again_ref, wq_hbm, wk_hbm, wv_hbm, bq_ref, bk_ref, bv_ref, cos_hbm, sin_hbm = refs[:9]
        refs = refs[9:]
    out_hbm = refs.pop(0)
    if with_qkv:
        q_hbm, k_hbm, v_hbm, kv_hbm = refs[:4]
        refs = refs[4:]
    w_full, o_full, hs, recv, xbuf, acc, wg, wu, wd, w_sems, in_sems, x_sems, o_sems, send_sems, recv_sems, out_sems, qkv_sems = refs
    rows, half = o_own.shape
    n_chunks, n_tiles = rows // chunk, wg_hbm.shape[2] // tile
    tp = lax.axis_index("tp")
    peer = {"tp": 1 - tp}
    own_cols = pl.ds(pl.multiple_of(tp * half, half), half)
    peer_cols = pl.ds(pl.multiple_of((1 - tp) * half, half), half)
    head_part, tail_part = pl.ds(0, head_rows), pl.ds(head_rows, rows - head_rows)
    def w_copies(i):
        c = pl.ds(pl.multiple_of(i * tile, tile), tile)
        return (
            pltpu.make_async_copy(wg_hbm.at[layer, :, c], wg.at[:, c], w_sems.at[i, 0]),
            pltpu.make_async_copy(wu_hbm.at[layer, :, c], wu.at[:, c], w_sems.at[i, 1]),
            pltpu.make_async_copy(wd_hbm.at[layer, c], wd.at[c], w_sems.at[i, 2]),
        )

    def chunk_rows(ci):
        return pl.ds(pl.multiple_of(ci * chunk, chunk), chunk)

    def x_copy(ci):
        return pltpu.make_async_copy(x_hbm.at[chunk_rows(ci)], xbuf.at[lax.rem(ci, 2)], x_sems.at[ci])

    def swap(ci):
        r = chunk_rows(ci)
        return pltpu.make_async_remote_copy(src_ref=hs.at[r], dst_ref=recv.at[r], send_sem=send_sems.at[ci], recv_sem=recv_sems.at[ci], device_id=peer, device_id_type=MESH)

    first = [
        pltpu.make_async_copy(w_out.at[layer], w_full.at[own_cols], in_sems.at[0]),
        pltpu.make_async_copy(w_peer, w_full.at[peer_cols], in_sems.at[1]),
        pltpu.make_async_copy(o_own, o_full.at[:, own_cols], in_sems.at[2]),
        pltpu.make_async_copy(o_head, o_full.at[head_part, peer_cols], in_sems.at[3]),
        x_copy(0),
    ]
    for copy in first:
        copy.start()
    barrier = pltpu.get_barrier_semaphore()
    pl.semaphore_signal(barrier, inc=1, device_id=peer, device_id_type=MESH)
    pl.semaphore_wait(barrier, 1)
    o_swap = pltpu.make_async_remote_copy(src_ref=o_own.at[tail_part], dst_ref=o_full.at[tail_part, own_cols], send_sem=o_sems.at[0], recv_sem=o_sems.at[1], device_id=peer, device_id_type=MESH)
    o_swap.start()
    for i in range(n_tiles):
        for copy in w_copies(i):
            copy.start()
    for copy in first:
        copy.wait()

    def run_chunk(ci, carry):
        r = chunk_rows(ci)

        @pl.when(ci == head_rows // chunk)
        def _():
            o_swap.wait()

        @pl.when(ci > 0)
        def _():
            x_copy(ci).wait()

        @pl.when(ci + 1 < n_chunks)
        def _():
            x_copy(ci + 1).start()

        prod = jnp.dot(o_full[r, :], w_full[...], preferred_element_type=jnp.float32)
        x1 = (xbuf[lax.rem(ci, 2)].astype(jnp.float32) + prod).astype(jnp.bfloat16)
        o_full[r, :] = x1
        hs[r, :] = rms_rows(x1.astype(jnp.float32), gain_ref[...].astype(jnp.float32)[layer:layer + 1])
        acc[...] = jnp.zeros(acc.shape, jnp.float32)

        def run_tile(i, c0):
            @pl.when(ci == 0)
            def _():
                for copy in w_copies(i):
                    copy.wait()

            c = pl.ds(pl.multiple_of(i * tile, tile), tile)
            normed = hs[r, :]
            gate = jnp.dot(normed, wg[:, c], preferred_element_type=jnp.float32)
            up = jnp.dot(normed, wu[:, c], preferred_element_type=jnp.float32)
            act = (gate * jax.nn.sigmoid(gate) * up).astype(jnp.bfloat16)
            acc[...] += jnp.dot(act, wd[c, :], preferred_element_type=jnp.float32)
            return c0

        lax.fori_loop(0, n_tiles, run_tile, 0)
        hs[r, :] = acc[...].astype(jnp.bfloat16)
        swap(ci).start()
        return carry

    lax.fori_loop(0, n_chunks, run_chunk, 0)

    if with_qkv:
        q_cols = wq_hbm.shape[2]
        kv_cols = q_cols + 2 * HEAD_DIM
        nxt = layer + 1
        b_q, b_k, b_v = (b[...].astype(jnp.float32)[nxt:nxt + 1] for b in (bq_ref, bk_ref, bv_ref))
        loads = [
            pltpu.make_async_copy(wq_hbm.at[nxt], w_full.at[:, pl.ds(0, q_cols)], qkv_sems.at[0]),
            pltpu.make_async_copy(wk_hbm.at[nxt], w_full.at[:, pl.ds(q_cols, HEAD_DIM)], qkv_sems.at[1]),
            pltpu.make_async_copy(wv_hbm.at[nxt], w_full.at[:, pl.ds(q_cols + HEAD_DIM, HEAD_DIM)], qkv_sems.at[2]),
        ]
        for ci in range(n_chunks):
            r = pl.ds(ci * chunk, chunk)
            at = ci * 2 * HEAD_DIM
            loads.append(pltpu.make_async_copy(cos_hbm.at[r], acc.at[:, pl.ds(at, HEAD_DIM)], qkv_sems.at[3 + 2 * ci]))
            loads.append(pltpu.make_async_copy(sin_hbm.at[r], acc.at[:, pl.ds(at + HEAD_DIM, HEAD_DIM)], qkv_sems.at[4 + 2 * ci]))
        for copy in loads:
            copy.start()
        for copy in loads:
            copy.wait()
    def out_copies(ci):
        r = chunk_rows(ci)
        copies = [pltpu.make_async_copy(o_full.at[r], out_hbm.at[r], out_sems.at[ci, 0])]
        if with_qkv:
            copies.append(pltpu.make_async_copy(hs.at[r, pl.ds(0, q_cols)], q_hbm.at[r], out_sems.at[ci, 1]))
            copies.append(pltpu.make_async_copy(hs.at[r, pl.ds(q_cols, HEAD_DIM)], k_hbm.at[r], out_sems.at[ci, 2]))
            copies.append(pltpu.make_async_copy(hs.at[r, pl.ds(q_cols + HEAD_DIM, HEAD_DIM)], v_hbm.at[r], out_sems.at[ci, 3]))
            copies.append(pltpu.make_async_copy(hs.at[r, pl.ds(q_cols, 2 * HEAD_DIM)], kv_hbm.at[r], out_sems.at[ci, 4]))
        return copies

    def finish_chunk(ci, carry):
        r = chunk_rows(ci)
        swap(ci).wait()
        total = hs[r, :].astype(jnp.float32) + recv[r, :].astype(jnp.float32)
        x2 = (o_full[r, :].astype(jnp.float32) + total).astype(jnp.bfloat16)
        o_full[r, :] = x2
        if with_qkv:
            at = ci * 2 * HEAD_DIM
            cos_tab = acc[:, pl.ds(pl.multiple_of(at, HEAD_DIM), HEAD_DIM)]
            sin_tab = acc[:, pl.ds(pl.multiple_of(at + HEAD_DIM, HEAD_DIM), HEAD_DIM)]
            normed = rms_rows(x2.astype(jnp.float32), again_ref[...].astype(jnp.float32)[nxt:nxt + 1])
            proj = jnp.dot(normed, w_full[:, :kv_cols], preferred_element_type=jnp.float32)

            def rope(cols, bias):
                block = proj[:, cols] + bias
                return (block * cos_tab + pltpu.roll(block, HEAD_DIM // 2, 1) * sin_tab).astype(jnp.bfloat16)

            for at in range(0, q_cols, HEAD_DIM):
                cols = slice(at, at + HEAD_DIM)
                hs[r, cols] = rope(cols, b_q[:, cols])
            k_cols, v_cols = slice(q_cols, q_cols + HEAD_DIM), slice(q_cols + HEAD_DIM, kv_cols)
            hs[r, k_cols] = rope(k_cols, b_k)
            hs[r, v_cols] = (proj[:, v_cols] + b_v).astype(jnp.bfloat16)
        for copy in out_copies(ci):
            copy.start()
        return carry

    lax.fori_loop(0, n_chunks, finish_chunk, 0)
    for ci in range(n_chunks):
        for copy in out_copies(ci):
            copy.wait()


def layer_tail(layer, o_own, o_head, x, gain, w_out, w_peer, wg, wu, wd, next_qkv, cid):
    rows, half = o_own.shape
    width = x.shape[1]
    cols = wg.shape[2]
    tile, chunk = 896, 256
    nt, nc = cols // tile, rows // chunk
    anys = pl.BlockSpec(memory_space=pl.ANY)
    bf = jnp.bfloat16
    dma = pltpu.SemaphoreType.DMA

    vm = pl.BlockSpec(memory_space=pltpu.VMEM)
    args = [o_own, o_head, x, gain, w_out, w_peer, wg, wu, wd]
    specs = [anys] * 3 + [vm] + [anys] * 5
    outs = [jax.ShapeDtypeStruct((rows, width), bf)]
    if next_qkv is not None:
        again, wq, wk, wv, bq, bk, bv, cos_tab, sin_tab = next_qkv
        args += list(next_qkv)
        specs += [vm] + [anys] * 3 + [vm] * 3 + [anys] * 2
        outs += [jax.ShapeDtypeStruct((rows, c), bf) for c in (wq.shape[2], HEAD_DIM, HEAD_DIM, 2 * HEAD_DIM)]
    return pl.pallas_call(
        functools.partial(tail_kernel, layer=layer, tile=tile, chunk=chunk, head_rows=o_head.shape[0], with_qkv=next_qkv is not None),
        in_specs=specs,
        out_specs=[anys] * len(outs),
        out_shape=outs,
        scratch_shapes=[
            pltpu.VMEM((2 * half, width), bf), pltpu.VMEM((rows, width), bf), pltpu.VMEM((rows, width), bf), pltpu.VMEM((rows, width), bf),
            pltpu.VMEM((2, chunk, width), bf), pltpu.VMEM((chunk, width), jnp.float32),
            pltpu.VMEM((width, cols), bf), pltpu.VMEM((width, cols), bf), pltpu.VMEM((cols, width), bf),
            dma((nt, 3)), dma((4,)), dma((nc,)), dma((2,)), dma((nc,)), dma((nc,)), dma((nc, 5)), dma((3 + 2 * nc,)),
        ],
        compiler_params=pltpu.CompilerParams(vmem_limit_bytes=67043328, collective_id=cid, has_side_effects=True),
        cost_estimate=pl.CostEstimate(flops=6 * rows * width * cols, bytes_accessed=6 * width * cols, transcendentals=0),
        name="tail",
    )(*args)


def solution(mesh):
    cp_size = mesh.shape["cp"]

    def local_step(x_in, positions, attn_gain, mlp_gain, w_query, b_query, w_key, b_key, w_value, b_value, w_out, w_gate, w_up, w_down):
        block_dev = x_in.shape[0]
        inv_freq = 1.0 / (1000000.0 ** (jnp.arange(0, HEAD_DIM, 2, dtype=jnp.float32) / HEAD_DIM))
        angles = positions.astype(jnp.float32)[:, None] * inv_freq[None, :]
        cos_half, sin_half = jnp.cos(angles), jnp.sin(angles)
        cos_tab = jnp.concatenate([cos_half, cos_half], axis=1)
        sin_tab = jnp.concatenate([-sin_half, sin_half], axis=1)
        qkv_args = (attn_gain, w_query, w_key, w_value, b_query, b_key, b_value, cos_tab, sin_tab)
        hidden, caches = x_in, []
        q, k, v, kv = qkv(hidden, *qkv_args)
        for layer, window_blocks in ((0, cp_size), (1, WINDOW // block_dev)):
            caches.append(k[:, None, :])
            caches.append(v[:, None, :])
            o, o_head, w_peer = attention(layer, q, kv, w_out, window_blocks, 512, 2 * layer)
            hidden, *rest = layer_tail(layer, o, o_head, hidden, mlp_gain, w_out, w_peer, w_gate, w_up, w_down, qkv_args if layer == 0 else None, 2 * layer + 1)
            if layer == 0:
                q, k, v, kv = rest
        return hidden, caches[0], caches[1], caches[2], caches[3]

    weight_col = P(None, None, "tp")
    bias_col = P(None, "tp")
    weight_row = P(None, "tp", None)
    replicated = P(None, None)
    cache_spec = P("cp", "tp", None)
    in_specs = (P("cp", None), P("cp"), replicated, replicated, weight_col, bias_col, weight_col, bias_col, weight_col, bias_col, weight_row, weight_col, weight_col, weight_row)
    out_specs = (P("cp", None), cache_spec, cache_spec, cache_spec, cache_spec)
    return jax.shard_map(local_step, mesh=mesh, in_specs=in_specs, out_specs=out_specs, check_vma=False)
```
